32 devices in a mesh: section: 4 (over y, core), fsdp: 8 (over z, x).
Axes of the slice: x: 2, y: 2, z: 4, core: 2. Of those that a mesh axis runs over, the one named last changes fastest.
Arguments:
- old_pieces: bfloat16 [4, 2, 16384, 1024], P('section', None, 'fsdp'), may hold values from -0.0625 to 0.0625
- section_inputs: bfloat16 [4, 4096, 8192], P('section', 'fsdp'), may hold values from -6 to 6
- old_section_of: int32 [8], replicated, may hold values from 0 to 3, as said below
- new_section_of: int32 [8], replicated, may hold values from 0 to 7, as said below
- old_order: int32 [8, 2], replicated, may hold values from 0 to 1, each once within a row
- new_order: int32 [8, 2], replicated, may hold values from 0 to 1, each once within a row
Outputs:
- new_shards: bfloat16 [4, 32768, 1024], P('section', 'fsdp')
- kv_out: bfloat16 [4, 4096, 2048], P('section', 'fsdp')
The draws below stay inside these ranges and needn't reach their ends.
Inputs may be any that keep to these rules, and one draw needn't show every extreme that they name: `old_section_of`: each old section holds exactly two layers. Each new section holds exactly one layer; the two layers of one old section have different values of new_section_of // 2.
All inputs are finite; a program needn't handle non-finite values.
Results may differ from the reference program's by a relative error of at most 0.001.
Values may be sent and summed in bfloat16 or wider, within the bound.
A program may use at most 192 MiB of HBM per device.

```python
import math
import jax
import jax.numpy as jnp
from jax import lax

D = 8192
HEAD_DIM = 128
TOK_DEV = 512
KVW = 1024
LAYERS = 8
SHARD = 4096
N_SECTION = 4
N_FSDP = 8


def layer_maps(key):
    section_count = N_SECTION
    keys = jax.random.split(jax.random.fold_in(key, 11), 6)
    members = jax.random.permutation(keys[0], 2 * section_count).astype(jnp.int32)
    old_section = (jnp.argsort(members) // 2).astype(jnp.int32)
    rows_first = jax.random.permutation(keys[1], section_count).astype(jnp.int32)
    relabel = jax.random.permutation(keys[2], section_count).astype(jnp.int32)
    offset_steps = jax.random.randint(keys[3], (), 1, section_count).astype(jnp.int32)
    relabel_inverse = jnp.argsort(relabel).astype(jnp.int32)
    rows_second = rows_first[relabel_inverse[(relabel + offset_steps) % section_count]]
    swapped = jax.random.randint(keys[4], (section_count,), 0, 2).astype(jnp.int32)
    layer_alpha = jnp.where(swapped == 0, members[0::2], members[1::2])
    layer_beta = jnp.where(swapped == 0, members[1::2], members[0::2])
    halves = jax.random.randint(keys[5], (section_count,), 0, 2).astype(jnp.int32)
    section_alpha = 2 * rows_first + halves[rows_first]
    section_beta = 2 * rows_second + 1 - halves[rows_second]
    new_section = jnp.zeros((2 * section_count,), jnp.int32).at[layer_alpha].set(section_alpha).at[layer_beta].set(section_beta)
    return (old_section, new_section)


def draw_old_section_of(key, part):
    return layer_maps(key)[0]


def draw_new_section_of(key, part):
    return layer_maps(key)[1]


def levels(stream_key, dims, shards, low, high):
    factor_of = 1.0
    for dim, parts in shards:
        heights = jax.random.uniform(jax.random.fold_in(jax.random.fold_in(stream_key, 6), dim), (parts,), jnp.float32, low / len(shards), high / len(shards))
        factor_of = factor_of * jnp.repeat(jnp.exp(heights), dims[dim] // parts).reshape((-1,) + (1,) * (len(dims) - 1 - dim))
    return factor_of


def noise(key, extent, deviation, most, shards=(), kind=jnp.bfloat16):
    level = levels(key, extent, shards, -0.22, 0.18) if shards else 1.0
    result = jax.random.normal(key, extent, jnp.float32) * deviation * level
    return jnp.minimum(jnp.maximum(result, -most), most).astype(kind)


def setup_inputs(seed: int = 0) -> dict:
    streams_of = jax.random.split(jax.random.key(seed), 7)
    return {
        "old_pieces": noise(streams_of[0], (N_SECTION, 2, 2 * D, KVW), D ** -0.5, 0.0625, ((0, 4), (2, 8))),
        "section_inputs": noise(streams_of[1], (N_SECTION, N_FSDP * TOK_DEV, D), 1.0, 6.0, ((0, 4), (1, 8))),
        "old_section_of": draw_old_section_of(jax.random.fold_in(streams_of[6], 71), 0),
        "new_section_of": draw_new_section_of(jax.random.fold_in(streams_of[6], 71), 0),
        "old_order": jax.vmap(lambda own: jax.random.permutation(own, 2))(jax.random.split(streams_of[4], LAYERS)).reshape((LAYERS, 2)).astype(jnp.int32),
        "new_order": jax.vmap(lambda own: jax.random.permutation(own, 2))(jax.random.split(streams_of[5], LAYERS)).reshape((LAYERS, 2)).astype(jnp.int32),
    }


def rotate_keys(values, positions):
    tok_rows = values.shape[0]
    heads = values.reshape(tok_rows, -1, HEAD_DIM)
    half_dim = HEAD_DIM // 2
    freq_index = jnp.arange(half_dim, dtype=jnp.float32)
    inverse_freq = jnp.exp(freq_index * (-2.0 * math.log(500000.0) / HEAD_DIM))
    angles = positions.astype(jnp.float32)[:, None] * inverse_freq[None, :]
    cosine = jnp.cos(angles)[:, None, :]
    sine = jnp.sin(angles)[:, None, :]
    lower = heads[..., :half_dim]
    upper = heads[..., half_dim:]
    turned = jnp.concatenate([lower * cosine - upper * sine, upper * cosine + lower * sine], axis=-1)
    return turned.reshape(tok_rows, -1)


def reference(old_pieces, section_inputs, old_section_of, new_section_of, old_order, new_order):
    layer_ids = jnp.arange(LAYERS, dtype=jnp.int32)
    group_size = N_FSDP // 2
    shard_list = []
    output_list = []
    for row_index in range(N_SECTION):
        shard_halves = []
        output_halves = []
        for half in range(2):
            layer_index = jnp.sum(jnp.where(new_section_of == 2 * row_index + half, layer_ids, 0)).astype(jnp.int32)
            old_section = old_section_of[layer_index]
            slot_index = jnp.sum(((old_section_of == old_section) & (layer_ids < layer_index)).astype(jnp.int32))
            flat_rows = old_pieces[old_section, slot_index]
            key_weight = lax.dynamic_slice_in_dim(flat_rows, (old_order[layer_index, 0] * D).astype(jnp.int32), D, 0)
            value_weight = lax.dynamic_slice_in_dim(flat_rows, (old_order[layer_index, 1] * D).astype(jnp.int32), D, 0)
            new_flat = jnp.where(new_order[layer_index, 0] == 0,
                                 jnp.concatenate([key_weight, value_weight], axis=0),
                                 jnp.concatenate([value_weight, key_weight], axis=0))
            shard_halves.append(new_flat.reshape(group_size, SHARD, KVW))
            tokens = section_inputs[row_index].reshape(group_size, 2, TOK_DEV, D)[:, half].reshape(group_size * TOK_DEV, D)
            keys = jnp.dot(tokens, key_weight, preferred_element_type=jnp.float32)
            values = jnp.dot(tokens, value_weight, preferred_element_type=jnp.float32)
            positions = jnp.arange(group_size * TOK_DEV, dtype=jnp.int32)
            joined = jnp.concatenate([rotate_keys(keys, positions), values], axis=-1).astype(jnp.bfloat16)
            output_halves.append(joined.reshape(group_size, TOK_DEV, 2 * KVW))
        shard_list.append(jnp.stack(shard_halves, axis=1).reshape(4 * D, KVW))
        output_list.append(jnp.stack(output_halves, axis=1).reshape(N_FSDP * TOK_DEV, 2 * KVW))
    return jnp.stack(shard_list), jnp.stack(output_list)
```

```python
import functools
import math

import jax
import jax.numpy as jnp
import numpy as np
from jax import lax
from jax.experimental import pallas as pl
from jax.experimental.pallas import tpu as pltpu
from jax.sharding import PartitionSpec as P


HEAD_DIM = 128


CHUNK = HEAD_DIM
MESH = pl.DeviceIdType.MESH
CROSS_LAG = 11
RETURN_LAG = 6
CHUNK_STEPS = 3
PIECES_PER_STEP = 3


def chain_kernel(
    block_rows, piece_rows,
    old_ref, tok_ref, old_sec, new_sec, old_ord, new_ord, freq_ref,
    shard_ref, kv_ref, relay_ref, middle_ref,
    oldv, send, keep, recv, held, forv, cross, tokv, cos_t, sin_t,
    relay_w, middle_w, sums, sumr, acc, kvst, shst,
    old_sem, sec_send_sem, sec_recv_sem, x_send_sem, x_recv_sem, own_send_sem, relay_sem,
    middle_sem, fwd_send_sem, ret_send_sem, cross_sem, tok_sem, piece_send_sem, piece_recv_sem,
    weight_sem, sum_send_sem, sum_recv_sem, kv_sem, shard_sem,
):
    rows = old_ref.shape[2]
    kv_width = old_ref.shape[3]
    tok_rows = tok_ref.shape[1]
    half_width = tok_ref.shape[2] // 2
    chunks = kv_width // CHUNK
    blocks = rows // block_rows
    steps = chunks * blocks
    pieces = tok_rows // piece_rows
    layers = old_sec.shape[0]

    sec = lax.axis_index("section")
    member = lax.axis_index("fsdp")
    z, x = member // 2, member % 2
    upper = z // 2
    inner = (z == 1) | (z == 2)
    outer = (z == 0) | (z == 3)
    side = z % 2
    across = {"fsdp": (3 - z) * 2 + x}
    beside = {"fsdp": (z + 1 - 2 * side) * 2 + x}
    partner = {"fsdp": z * 2 + 1 - x}

    def section_at(offset):
        flip_core, flip_y = offset % 2, offset // 2
        core, y = sec % 2, sec // 2
        core = 1 - core if flip_core else core
        y = 1 - y if flip_y else y
        return y * 2 + core

    barrier = pltpu.get_barrier_semaphore()
    for offset in (1, 2, 3):
        pl.semaphore_signal(
            barrier, inc=1, device_id={"section": section_at(offset)}, device_id_type=MESH
        )
    pl.semaphore_signal(barrier, inc=1, device_id=partner, device_id_type=MESH)
    pl.semaphore_signal(barrier, inc=1, device_id=beside, device_id_type=MESH)

    @pl.when(inner)
    def _():
        pl.semaphore_signal(barrier, inc=1, device_id=across, device_id_type=MESH)

    def old_load(t):
        j, b = t // blocks, t % blocks
        return pltpu.make_async_copy(
            old_ref.at[0, :, pl.ds(b * block_rows, block_rows), pl.ds(j * CHUNK, CHUNK)],
            oldv.at[t % 2],
            old_sem.at[t % 2],
        )

    def tok_load(which):
        column = (side if which == 0 else 1 - side) * half_width
        return pltpu.make_async_copy(
            tok_ref.at[0, :, pl.ds(column, half_width)], tokv.at[which], tok_sem.at[which]
        )

    old_load(0).start()
    old_load(1).start()
    tok_load(0).start()
    tok_load(1).start()

    target_low = jnp.int32(0)
    own_from, foreign_from = jnp.int32(0), jnp.int32(0)
    old_first, new_first = jnp.int32(0), jnp.int32(0)
    seen = jnp.int32(0)
    for layer in range(layers):
        here = old_sec[layer] == sec
        place = new_sec[layer]
        target_low = jnp.where(here & (seen == 0), place // 2, target_low)
        seen = jnp.where(here, 1, seen)
        own_from = jnp.where(place == 2 * sec + x, old_sec[layer], own_from)
        foreign_from = jnp.where(place == 2 * sec + 1 - x, old_sec[layer], foreign_from)
        old_first = jnp.where(place == 2 * sec + x, old_ord[layer, 0], old_first)
        new_first = jnp.where(place == 2 * sec + x, new_ord[layer, 0], new_first)
    flipped = old_first != new_first
    own_is_key = old_first == upper

    @pl.when(inner)
    def _():
        pl.semaphore_wait(barrier, 6)

    @pl.when(outer)
    def _():
        pl.semaphore_wait(barrier, 5)

    def place_of(t):
        return t // blocks, pl.ds(pl.multiple_of((t % blocks) * block_rows, block_rows), block_rows)

    def sec_copy(t, offset):
        return pltpu.make_async_remote_copy(
            src_ref=send.at[t % 2, offset - 1],
            dst_ref=recv.at[t, offset - 1],
            send_sem=sec_send_sem.at[t % 2, offset - 1],
            recv_sem=sec_recv_sem.at[t, offset - 1],
            device_id={"section": section_at(offset)},
            device_id_type=MESH,
        )

    def x_copy(t):
        j, at = place_of(t)
        return pltpu.make_async_remote_copy(
            src_ref=forv.at[t % 2],
            dst_ref=held.at[j, x, at],
            send_sem=x_send_sem.at[t % 2],
            recv_sem=x_recv_sem.at[t],
            device_id=partner,
            device_id_type=MESH,
        )

    def own_copy(t, to_middle):
        j, at = place_of(t)
        return pltpu.make_async_remote_copy(
            src_ref=held.at[j, :, at],
            dst_ref=(middle_ref if to_middle else relay_ref).at[j, :, at],
            send_sem=own_send_sem.at[t],
            recv_sem=(middle_sem if to_middle else relay_sem).at[t],
            device_id=across if to_middle else beside,
            device_id_type=MESH,
        )

    def cross_copy(t, forward):
        j, at = place_of(t)
        return pltpu.make_async_remote_copy(
            src_ref=(relay_ref if forward else middle_ref).at[j, :, at],
            dst_ref=cross.at[j, :, at],
            send_sem=(fwd_send_sem if forward else ret_send_sem).at[t],
            recv_sem=cross_sem.at[t],
            device_id=across if forward else beside,
            device_id_type=MESH,
        )

    def piece_copy(p):
        at = pl.ds(pl.multiple_of(p * piece_rows, piece_rows), piece_rows)
        column = (1 - side) * half_width
        return pltpu.make_async_remote_copy(
            src_ref=tok_ref.at[0, at, pl.ds(column, half_width)],
            dst_ref=tokv.at[2, at],
            send_sem=piece_send_sem.at[p],
            recv_sem=piece_recv_sem.at[p],
            device_id=beside,
            device_id_type=MESH,
        )

    def sum_copy(j, which):
        return pltpu.make_async_remote_copy(
            src_ref=sums.at[j % 2, which],
            dst_ref=sumr.at[j, which],
            send_sem=sum_send_sem.at[j % 2, which],
            recv_sem=sum_recv_sem.at[j, which],
            device_id=beside,
            device_id_type=MESH,
        )

    def weight_load(j, which):
        return pltpu.make_async_copy(
            (middle_ref if which else relay_ref).at[j],
            middle_w if which else relay_w,
            weight_sem.at[which],
        )

    def kv_store(j, which):
        return pltpu.make_async_copy(
            kvst.at[j % 2, which],
            kv_ref.at[0, :, pl.ds(which * kv_width + j * CHUNK, CHUNK)],
            kv_sem.at[j % 2, which],
        )

    def shard_store(j):
        return pltpu.make_async_copy(
            shst.at[j % 2],
            shard_ref.at[:, :, pl.ds(j * CHUNK, CHUNK)],
            shard_sem.at[j % 2],
        )

    tile = min(256, tok_rows)
    tiles = tok_rows // tile

    def product(which, weights, at):
        near = jnp.dot(
            tokv[which, at, pl.ds(0, rows)], weights[0], preferred_element_type=jnp.float32
        )
        far = jnp.dot(
            tokv[which, at, pl.ds(rows, rows)], weights[1], preferred_element_type=jnp.float32
        )
        return near + far

    def each_tile(body):
        def run(i, carry):
            body(pl.ds(pl.multiple_of(i * tile, tile), tile))
            return carry

        lax.fori_loop(0, tiles, run, 0)

    def angles():
        part = min(64, tok_rows)

        def run(i, carry):
            at = pl.ds(pl.multiple_of(i * part, part), part)
            base = z * tok_rows + i * part
            position = base + lax.broadcasted_iota(jnp.int32, (part, CHUNK), 0)
            angle = position.astype(jnp.float32) * freq_ref[...]
            lane = lax.broadcasted_iota(jnp.int32, (part, CHUNK), 1)
            cos_t[at] = jnp.cos(angle)
            sine = jnp.sin(angle)
            sin_t[at] = jnp.where(lane < CHUNK // 2, -sine, sine)
            return carry

        lax.fori_loop(0, tok_rows // part, run, 0)

    first_compute = steps + CROSS_LAG - CHUNK_STEPS * (chunks - 1)

    def compute_own(j):
        @pl.when(j == 0)
        def _():
            tok_load(0).wait()
            tok_load(1).wait()

            @pl.when(inner)
            def _():
                def wait_piece(p, carry):
                    piece_copy(p).wait_recv()
                    return carry

                lax.fori_loop(0, pieces, wait_piece, 0)

        @pl.when(inner)
        def _():
            @pl.when(j >= 2)
            def _():
                sum_copy(j - 2, 0).wait_send()

            def foreign(at):
                sums[j % 2, 0, at] = product(2, held.at[j], at)

            each_tile(foreign)
            sum_copy(j, 0).start()
            weight_load(j, 0).wait()
            weight_load(j, 1).wait()

            def both(at):
                acc[0, at] = product(0, held.at[j], at) + product(1, relay_w, at)
                acc[1, at] = product(1, middle_w, at)

            each_tile(both)

        @pl.when(outer)
        def _():
            def mine(at):
                acc[0, at] = product(0, held.at[j], at)

            each_tile(mine)

    def compute_cross(j):
        for b in range(blocks):
            cross_copy(j * blocks + b, True).wait_recv()

        @pl.when(inner)
        def _():
            @pl.when(j >= 2)
            def _():
                sum_copy(j - 2, 1).wait_send()

            def foreign(at):
                sums[j % 2, 1, at] = product(2, cross.at[j], at)

            each_tile(foreign)
            sum_copy(j, 1).start()

            def mine(at):
                acc[1, at] = acc[1, at] + product(0, cross.at[j], at)

            each_tile(mine)

        @pl.when(outer)
        def _():
            def mine(at):
                acc[1, at] = product(0, cross.at[j], at)

            each_tile(mine)

        @pl.when(j >= 2)
        def _():
            shard_store(j - 2).wait()
            kv_store(j - 2, 0).wait()
            kv_store(j - 2, 1).wait()

        shst[j % 2] = jnp.where(flipped, cross[j], held[j])
        shard_store(j).start()

        @pl.when(outer)
        def _():
            for which in range(2):
                sum_copy(j, which).wait_recv()
                acc[which] = acc[which] + sumr[j, which]

        first, second = acc[0], acc[1]
        keys = jnp.where(own_is_key, first, second)
        values = jnp.where(own_is_key, second, first)
        turned = keys * cos_t[...] + pltpu.roll(keys, CHUNK // 2, 1) * sin_t[...]
        kvst[j % 2, 0] = turned.astype(kvst.dtype)
        kvst[j % 2, 1] = values.astype(kvst.dtype)
        kv_store(j, 0).start()
        kv_store(j, 1).start()

    def step(tau, carry):
        @pl.when(tau < steps)
        def _():
            t = tau
            old_load(t).wait()

            @pl.when(t >= 2)
            def _():
                for offset in (1, 2, 3):
                    sec_copy(t - 2, offset).wait_send()

            low, high = oldv[t % 2, 0], oldv[t % 2, 1]
            for offset in (2, 3, 1):
                send[t % 2, offset - 1] = jnp.where(target_low == section_at(offset), low, high)
            keep[t % 4] = jnp.where(target_low == sec, low, high)
            for offset in (2, 3, 1):
                sec_copy(t, offset).start()

            @pl.when(t + 2 < steps)
            def _():
                old_load(t + 2).start()

        @pl.when(outer)
        def _():
            for k in range(PIECES_PER_STEP):
                p = tau * PIECES_PER_STEP + k

                @pl.when(p < pieces)
                def _():
                    piece_copy(p).start()

        @pl.when((tau >= 2) & (tau < steps + 2))
        def _():
            t = tau - 2
            for offset in (1, 2, 3):
                sec_copy(t, offset).wait_recv()

            @pl.when(t >= 2)
            def _():
                x_copy(t - 2).wait_send()

            j, at = place_of(t)
            own, foreign = keep[t % 4], keep[t % 4]
            for offset in (1, 2, 3):
                arrived = recv[t, offset - 1]
                own = jnp.where(own_from == section_at(offset), arrived, own)
                foreign = jnp.where(foreign_from == section_at(offset), arrived, foreign)
            forv[t % 2] = foreign
            held[j, x, at] = own
            x_copy(t).start()

        @pl.when((tau >= 3) & (tau < steps + 3))
        def _():
            t = tau - 3
            x_copy(t).wait_recv()

            @pl.when(outer)
            def _():
                own_copy(t, False).start()

            @pl.when(inner)
            def _():
                own_copy(t, True).start()

        @pl.when(inner & (tau >= RETURN_LAG) & (tau < steps + RETURN_LAG))
        def _():
            t = tau - RETURN_LAG
            own_copy(t, True).wait_recv()
            cross_copy(t, False).start()

        @pl.when(inner & (tau >= CROSS_LAG) & (tau < steps + CROSS_LAG))
        def _():
            t = tau - CROSS_LAG
            own_copy(t, False).wait_recv()
            cross_copy(t, True).start()

        @pl.when(tau == 4)
        def _():
            angles()

        since = tau - first_compute + 1
        j = since // CHUNK_STEPS
        phase = since % CHUNK_STEPS
        live = (since >= 0) & (j < chunks)

        @pl.when(inner & live & (phase == 0))
        def _():
            weight_load(j, 0).start()
            weight_load(j, 1).start()

        @pl.when(live & (phase == 1))
        def _():
            compute_own(j)

        @pl.when(live & (phase == 2))
        def _():
            compute_cross(j)

        return carry

    lax.fori_loop(0, steps + CROSS_LAG + 2, step, 0)

    for t in (steps - 2, steps - 1):
        for offset in (1, 2, 3):
            sec_copy(t, offset).wait_send()
        x_copy(t).wait_send()

    def drain(t, carry):
        @pl.when(outer)
        def _():
            own_copy(t, False).wait_send()

        @pl.when(inner)
        def _():
            own_copy(t, True).wait_send()
            cross_copy(t, False).wait_send()
            cross_copy(t, True).wait_send()

        return carry

    lax.fori_loop(0, steps, drain, 0)

    @pl.when(outer)
    def _():
        def drain_piece(p, carry):
            piece_copy(p).wait_send()
            return carry

        lax.fori_loop(0, pieces, drain_piece, 0)

    for j in (chunks - 2, chunks - 1):
        @pl.when(inner)
        def _():
            for which in range(2):
                sum_copy(j, which).wait_send()

        for which in range(2):
            kv_store(j, which).wait()
        shard_store(j).wait()


def per_device_chain(old_pieces, section_inputs, old_sec, new_sec, old_ord, new_ord):
    _, layers_held, rows, kv_width = old_pieces.shape
    _, tok_rows, width = section_inputs.shape
    chunks = kv_width // CHUNK
    block_rows = rows // 4
    steps = chunks * 4
    piece_rows = tok_rows // 32
    pieces = tok_rows // piece_rows
    half_dim = HEAD_DIM // 2
    index = np.arange(half_dim, dtype=np.float32)
    factor = np.float32(-2.0 * math.log(500000.0) / HEAD_DIM)
    freq = np.exp((index * factor).astype(np.float64)).astype(np.float32)
    freq = jnp.asarray(np.concatenate([freq, freq])[None])
    kind = old_pieces.dtype
    dma = pltpu.SemaphoreType.DMA
    hbm = pl.BlockSpec(memory_space=pltpu.HBM)
    smem = pl.BlockSpec(memory_space=pltpu.SMEM)
    shard, kv, _, _ = pl.pallas_call(
        functools.partial(chain_kernel, block_rows, piece_rows),
        out_shape=(
            jax.ShapeDtypeStruct((2, rows, kv_width), kind),
            jax.ShapeDtypeStruct((1, tok_rows, 2 * kv_width), kind),
            jax.ShapeDtypeStruct((chunks, 2, rows, CHUNK), kind),
            jax.ShapeDtypeStruct((chunks, 2, rows, CHUNK), kind),
        ),
        in_specs=[hbm, hbm, smem, smem, smem, smem, pl.BlockSpec(memory_space=pltpu.VMEM)],
        out_specs=(hbm, hbm, hbm, hbm),
        scratch_shapes=[
            pltpu.VMEM((2, layers_held, block_rows, CHUNK), kind),
            pltpu.VMEM((2, 3, block_rows, CHUNK), kind),
            pltpu.VMEM((4, block_rows, CHUNK), kind),
            pltpu.VMEM((steps, 3, block_rows, CHUNK), kind),
            pltpu.VMEM((chunks, 2, rows, CHUNK), kind),
            pltpu.VMEM((2, block_rows, CHUNK), kind),
            pltpu.VMEM((chunks, 2, rows, CHUNK), kind),
            pltpu.VMEM((3, tok_rows, width // 2), kind),
            pltpu.VMEM((tok_rows, CHUNK), jnp.float32),
            pltpu.VMEM((tok_rows, CHUNK), jnp.float32),
            pltpu.VMEM((2, rows, CHUNK), kind),
            pltpu.VMEM((2, rows, CHUNK), kind),
            pltpu.VMEM((2, 2, tok_rows, CHUNK), jnp.float32),
            pltpu.VMEM((chunks, 2, tok_rows, CHUNK), jnp.float32),
            pltpu.VMEM((2, tok_rows, CHUNK), jnp.float32),
            pltpu.VMEM((2, 2, tok_rows, CHUNK), kind),
            pltpu.VMEM((2, 2, rows, CHUNK), kind),
            dma((2,)),
            dma((2, 3)),
            dma((steps, 3)),
            dma((2,)),
            dma((steps,)),
            dma((steps,)),
            dma((steps,)),
            dma((steps,)),
            dma((steps,)),
            dma((steps,)),
            dma((steps,)),
            dma((2,)),
            dma((pieces,)),
            dma((pieces,)),
            dma((2,)),
            dma((2, 2)),
            dma((chunks, 2)),
            dma((2, 2)),
            dma((2,)),
        ],
        compiler_params=pltpu.CompilerParams(
            collective_id=0, has_side_effects=True, vmem_limit_bytes=60 * 2**20
        ),
    )(old_pieces, section_inputs, old_sec, new_sec, old_ord, new_ord, freq)
    return shard.reshape(1, 2 * rows, kv_width), kv


def from_partner(block, axis, stride):
    count = lax.axis_size(axis)
    route = []
    for low in range(count):
        high = low | 1 << stride
        if high != low and high < count:
            route += [(low, high), (high, low)]
    return lax.ppermute(block, axis, route)


def from_offset(block, axis, offset):
    count = lax.axis_size(axis)
    return lax.ppermute(block, axis, [(i, i ^ offset) for i in range(count)])


def rotate_keys(values, positions):
    tok_rows = values.shape[0]
    heads = values.reshape(tok_rows, -1, HEAD_DIM)
    half_dim = HEAD_DIM // 2
    freq_index = jnp.arange(half_dim, dtype=jnp.float32)
    inverse_freq = jnp.exp(freq_index * (-2.0 * math.log(500000.0) / HEAD_DIM))
    angles = positions.astype(jnp.float32)[:, None] * inverse_freq[None, :]
    cosine = jnp.cos(angles)[:, None, :]
    sine = jnp.sin(angles)[:, None, :]
    lower = heads[..., :half_dim]
    upper = heads[..., half_dim:]
    turned = jnp.concatenate(
        [lower * cosine - upper * sine, upper * cosine + lower * sine], axis=-1
    )
    return turned.reshape(tok_rows, -1)


def pick_entry(table, index_value):
    positions = jnp.arange(table.shape[0], dtype=jnp.int32)
    return jnp.sum(jnp.where(positions == index_value, table, 0))


def pick_row(table, index_value):
    positions = jnp.arange(table.shape[0], dtype=jnp.int32)[:, None]
    return jnp.sum(jnp.where(positions == index_value, table, 0), axis=0)


def chunk_columns(kv_width):
    heads = kv_width // HEAD_DIM
    edge = [1, 1] if heads >= 4 else []
    middle = heads - len(edge)
    sizes = [2] * (middle // 2) + [1] * (middle % 2) + edge
    starts = [sum(sizes[:i]) for i in range(len(sizes))]
    return [(s * HEAD_DIM, n * HEAD_DIM) for s, n in zip(starts, sizes)]


def per_device(old_pieces, section_inputs, old_section_of, new_section_of, old_order, new_order):
    section_count = lax.axis_size("section")
    member_count = lax.axis_size("fsdp")
    digit_count = member_count.bit_length() - 1
    row_index = lax.axis_index("section")
    member = lax.axis_index("fsdp")
    parity = member % 2
    layer_total = old_section_of.shape[0]
    layer_ids = jnp.arange(layer_total, dtype=jnp.int32)
    in_row = old_section_of == row_index
    layer_low = jnp.min(jnp.where(in_row, layer_ids, layer_total))
    layer_high = jnp.max(jnp.where(in_row, layer_ids, -1))
    target_low = pick_entry(new_section_of, layer_low) // 2
    layer_own = jnp.sum(jnp.where(new_section_of == 2 * row_index + parity, layer_ids, 0))
    layer_foreign = jnp.sum(jnp.where(new_section_of == 2 * row_index + 1 - parity, layer_ids, 0))
    source_own = pick_entry(old_section_of, layer_own)
    source_foreign = pick_entry(old_section_of, layer_foreign)
    pieces = old_pieces[0]
    tokens = section_inputs[0]
    tok_rows, _ = tokens.shape
    shard_rows, kv_width = 2 * pieces.shape[1], pieces.shape[2]
    own_bits = {digit: member // 2**digit % 2 for digit in range(1, digit_count)}
    own_old = pick_row(old_order, layer_own)
    own_new = pick_row(new_order, layer_own)
    flipped = own_old[0] != own_new[0]
    group_digits = digit_count - 1
    low_count = group_digits // 2
    high_digits = list(range(low_count + 1, digit_count))
    low_digits = list(range(1, low_count + 1))
    top_bit = own_bits[digit_count - 1]

    def to_groups(low, high):
        sources = []
        for offset in range(section_count):
            chosen = jnp.where(target_low == row_index ^ offset, low, high)
            if offset:
                chosen = from_offset(chosen, "section", offset)
            sources.append(chosen)
        (own_from, foreign_from, here, side), sources = lax.optimization_barrier(
            ((source_own, source_foreign, row_index, parity), sources)
        )
        own, foreign = sources[0], sources[0]
        for offset in range(1, section_count):
            own = jnp.where(own_from == here ^ offset, sources[offset], own)
            foreign = jnp.where(foreign_from == here ^ offset, sources[offset], foreign)
        partner = from_partner(foreign, "fsdp", 0)
        lower = jnp.where(side == 0, own, partner)
        upper = jnp.where(side == 0, partner, own)
        return jnp.concatenate([lower, upper], axis=-2)

    def gather_high(block):
        blocks = [block]
        for digit in high_digits:
            blocks += [from_partner(held, "fsdp", digit) for held in blocks]
        return blocks

    block_digits = high_digits[:-1]
    place_digits = block_digits[::-1] + low_digits[::-1]

    def pick_columns(flips):
        column = 0
        for digit in place_digits:
            column = 2 * column + (own_bits[digit] ^ flips[digit])
        return lax.dynamic_slice_in_dim(tokens, column * shard_rows, shard_rows, axis=1)

    row_cuts = 4 if tok_rows % 64 == 0 else 1
    token_blocks = {}
    for number in range(2 ** len(block_digits)):
        flips = {digit: number >> place & 1 for place, digit in enumerate(block_digits)}
        pending = {}
        for want in range(2**low_count):
            low_flips = {digit: want >> place & 1 for place, digit in enumerate(low_digits)}
            pending[want] = pick_columns({**flips, **low_flips})
        for place, digit in enumerate(low_digits):
            moved = dict(pending)
            for want in range(2**low_count):
                if want >> place & 1:
                    cuts = jnp.split(pending[want], row_cuts, axis=0)
                    cuts = [from_partner(cut, "fsdp", digit) for cut in cuts]
                    moved[want] = jnp.concatenate(cuts, axis=0)
            pending = moved
        for want in range(2**low_count):
            token_blocks[want, number] = pending[want]

    def project(blocks):
        sums = []
        for want in reversed(range(2**low_count)):
            for number, block in enumerate(blocks):
                product = jnp.dot(
                    token_blocks[want, number], block, preferred_element_type=jnp.float32
                )
                total = total + product if number else product
            sums.append(total)
        sums = sums[::-1]
        for place in reversed(range(low_count)):
            half = len(sums) // 2
            sums = [
                kept + from_partner(sent, "fsdp", low_digits[place])
                for kept, sent in zip(sums[:half], sums[half:])
            ]
        return sums[0]

    positions = member // 2 * tok_rows + jnp.arange(tok_rows, dtype=jnp.int32)
    shard_parts, key_parts, value_parts = [], [], []
    for number, (start, width) in enumerate(chunk_columns(kv_width)):
        part = lax.slice_in_dim(pieces, start, start + width, axis=2)
        if number == 0:
            crossed = jnp.stack(gather_high(part), axis=1)
            held = to_groups(crossed[0], crossed[1])
            blocks = [held[i] for i in range(held.shape[0])]
        else:
            blocks = gather_high(to_groups(part[0], part[1]))
        half = len(blocks) // 2
        near = project(blocks[:half])
        far = project(blocks[half:])
        shard_parts.append(jnp.where(flipped, blocks[half], blocks[0]))
        keys = jnp.where(own_old[0] == top_bit, near, far)
        values = jnp.where(own_old[1] == top_bit, near, far)
        key_parts.append(rotate_keys(keys, positions).astype(jnp.bfloat16))
        value_parts.append(values.astype(jnp.bfloat16))
    new_shard = jnp.concatenate(shard_parts, axis=1)
    joined = jnp.concatenate(key_parts + value_parts, axis=1)
    return (new_shard[None], joined[None])


def solution(mesh):
    in_specs = (P("section", None, "fsdp", None), P("section", "fsdp", None), P(), P(), P(), P())
    out_specs = (P("section", "fsdp", None), P("section", "fsdp", None))

    if dict(mesh.shape) == {"section": 4, "fsdp": 8}:
        return jax.shard_map(
            per_device_chain, mesh=mesh, in_specs=in_specs, out_specs=out_specs, check_vma=False
        )

    return jax.shard_map(
        per_device, mesh=mesh, in_specs=in_specs, out_specs=out_specs, check_vma=False
    )
```

```python
import functools
import math

import jax
import jax.numpy as jnp
import numpy as np
from jax import lax
from jax.experimental import pallas as pl
from jax.experimental.pallas import tpu as pltpu
from jax.sharding import PartitionSpec as P


HEAD_DIM = 128


CHUNK = HEAD_DIM
MESH = pl.DeviceIdType.MESH
CROSS_LAG = 11
RETURN_LAG = 6
CHUNK_STEPS = 3
PIECES_PER_STEP = 3


def chain_kernel(
    block_rows, piece_rows,
    old_ref, tok_ref, old_sec, new_sec, old_ord, new_ord, freq_ref,
    shard_ref, kv_ref, relay_ref, middle_ref,
    oldv, send, keep, recv, held, forv, cross, tokv, cos_t, sin_t,
    relay_w, middle_w, sums, sumr, acc,
    old_sem, sec_send_sem, sec_recv_sem, x_send_sem, x_recv_sem, own_send_sem, relay_sem,
    middle_sem, fwd_send_sem, ret_send_sem, cross_sem, tok_sem, piece_send_sem, piece_recv_sem,
    weight_sem, sum_send_sem, sum_recv_sem,
):
    rows = old_ref.shape[2]
    kv_width = old_ref.shape[3]
    tok_rows = tok_ref.shape[1]
    half_width = tok_ref.shape[2] // 2
    chunks = kv_width // CHUNK
    blocks = rows // block_rows
    steps = chunks * blocks
    pieces = tok_rows // piece_rows
    layers = old_sec.shape[0]

    sec = lax.axis_index("section")
    member = lax.axis_index("fsdp")
    z, x = member // 2, member % 2
    upper = z // 2
    inner = (z == 1) | (z == 2)
    outer = (z == 0) | (z == 3)
    side = z % 2
    across = {"fsdp": (3 - z) * 2 + x}
    beside = {"fsdp": (z + 1 - 2 * side) * 2 + x}
    partner = {"fsdp": z * 2 + 1 - x}

    def section_at(offset):
        flip_core, flip_y = offset % 2, offset // 2
        core, y = sec % 2, sec // 2
        core = 1 - core if flip_core else core
        y = 1 - y if flip_y else y
        return y * 2 + core

    barrier = pltpu.get_barrier_semaphore()
    for offset in (1, 2, 3):
        pl.semaphore_signal(
            barrier, inc=1, device_id={"section": section_at(offset)}, device_id_type=MESH
        )
    pl.semaphore_signal(barrier, inc=1, device_id=partner, device_id_type=MESH)
    pl.semaphore_signal(barrier, inc=1, device_id=beside, device_id_type=MESH)

    @pl.when(inner)
    def _():
        pl.semaphore_signal(barrier, inc=1, device_id=across, device_id_type=MESH)

    def old_load(t):
        j, b = t // blocks, t % blocks
        return pltpu.make_async_copy(
            old_ref.at[0, :, pl.ds(b * block_rows, block_rows), pl.ds(j * CHUNK, CHUNK)],
            oldv.at[t % 2],
            old_sem.at[t % 2],
        )

    def tok_load(which):
        column = (side if which == 0 else 1 - side) * half_width
        return pltpu.make_async_copy(
            tok_ref.at[0, :, pl.ds(column, half_width)], tokv.at[which], tok_sem.at[which]
        )

    old_load(0).start()
    old_load(1).start()
    tok_load(0).start()
    tok_load(1).start()

    target_low = jnp.int32(0)
    own_from, foreign_from = jnp.int32(0), jnp.int32(0)
    old_first, new_first = jnp.int32(0), jnp.int32(0)
    seen = jnp.int32(0)
    for layer in range(layers):
        here = old_sec[layer] == sec
        place = new_sec[layer]
        target_low = jnp.where(here & (seen == 0), place // 2, target_low)
        seen = jnp.where(here, 1, seen)
        own_from = jnp.where(place == 2 * sec + x, old_sec[layer], own_from)
        foreign_from = jnp.where(place == 2 * sec + 1 - x, old_sec[layer], foreign_from)
        old_first = jnp.where(place == 2 * sec + x, old_ord[0, layer], old_first)
        new_first = jnp.where(place == 2 * sec + x, new_ord[0, layer], new_first)
    flipped = old_first != new_first
    own_is_key = old_first == upper

    @pl.when(inner)
    def _():
        pl.semaphore_wait(barrier, 6)

    @pl.when(outer)
    def _():
        pl.semaphore_wait(barrier, 5)

    def place_of(t):
        return t // blocks, pl.ds(pl.multiple_of((t % blocks) * block_rows, block_rows), block_rows)

    def sec_copy(t, offset):
        return pltpu.make_async_remote_copy(
            src_ref=send.at[t % 2, offset - 1],
            dst_ref=recv.at[t, offset - 1],
            send_sem=sec_send_sem.at[t % 2, offset - 1],
            recv_sem=sec_recv_sem.at[t, offset - 1],
            device_id={"section": section_at(offset)},
            device_id_type=MESH,
        )

    def x_copy(t):
        j, at = place_of(t)
        return pltpu.make_async_remote_copy(
            src_ref=forv.at[t % 2],
            dst_ref=held.at[j, x, at],
            send_sem=x_send_sem.at[t % 2],
            recv_sem=x_recv_sem.at[t],
            device_id=partner,
            device_id_type=MESH,
        )

    def own_copy(t, to_middle):
        j, at = place_of(t)
        return pltpu.make_async_remote_copy(
            src_ref=held.at[j, :, at],
            dst_ref=(middle_ref if to_middle else relay_ref).at[j, :, at],
            send_sem=own_send_sem.at[t],
            recv_sem=(middle_sem if to_middle else relay_sem).at[t],
            device_id=across if to_middle else beside,
            device_id_type=MESH,
        )

    def cross_copy(t, forward):
        j, at = place_of(t)
        return pltpu.make_async_remote_copy(
            src_ref=(relay_ref if forward else middle_ref).at[j, :, at],
            dst_ref=cross.at[j, :, at],
            send_sem=(fwd_send_sem if forward else ret_send_sem).at[t],
            recv_sem=cross_sem.at[t],
            device_id=across if forward else beside,
            device_id_type=MESH,
        )

    def piece_copy(p):
        at = pl.ds(pl.multiple_of(p * piece_rows, piece_rows), piece_rows)
        column = (1 - side) * half_width
        return pltpu.make_async_remote_copy(
            src_ref=tok_ref.at[0, at, pl.ds(column, half_width)],
            dst_ref=tokv.at[2, at],
            send_sem=piece_send_sem.at[p],
            recv_sem=piece_recv_sem.at[p],
            device_id=beside,
            device_id_type=MESH,
        )

    def sum_copy(j, which):
        return pltpu.make_async_remote_copy(
            src_ref=sums.at[j % 2, which],
            dst_ref=sumr.at[j, which],
            send_sem=sum_send_sem.at[j % 2, which],
            recv_sem=sum_recv_sem.at[j, which],
            device_id=beside,
            device_id_type=MESH,
        )

    def weight_load(j, which):
        return pltpu.make_async_copy(
            (middle_ref if which else relay_ref).at[j],
            middle_w if which else relay_w,
            weight_sem.at[which],
        )

    tile = min(256, tok_rows)
    tiles = tok_rows // tile

    def product(which, weights, at):
        near = jnp.dot(
            tokv[which, at, pl.ds(0, rows)], weights[0], preferred_element_type=jnp.float32
        )
        far = jnp.dot(
            tokv[which, at, pl.ds(rows, rows)], weights[1], preferred_element_type=jnp.float32
        )
        return near + far

    def each_tile(body):
        def run(i, carry):
            body(pl.ds(pl.multiple_of(i * tile, tile), tile))
            return carry

        lax.fori_loop(0, tiles, run, 0)

    def angles():
        part = min(64, tok_rows)

        def run(i, carry):
            at = pl.ds(pl.multiple_of(i * part, part), part)
            base = z * tok_rows + i * part
            position = base + lax.broadcasted_iota(jnp.int32, (part, CHUNK), 0)
            angle = position.astype(jnp.float32) * freq_ref[...]
            lane = lax.broadcasted_iota(jnp.int32, (part, CHUNK), 1)
            cos_t[at] = jnp.cos(angle)
            sine = jnp.sin(angle)
            sin_t[at] = jnp.where(lane < CHUNK // 2, -sine, sine)
            return carry

        lax.fori_loop(0, tok_rows // part, run, 0)

    first_compute = steps + CROSS_LAG - CHUNK_STEPS * (chunks - 1)

    def compute_own(j):
        @pl.when(j == 0)
        def _():
            tok_load(0).wait()
            tok_load(1).wait()

            @pl.when(inner)
            def _():
                def wait_piece(p, carry):
                    piece_copy(p).wait_recv()
                    return carry

                lax.fori_loop(0, pieces, wait_piece, 0)

        @pl.when(inner)
        def _():
            @pl.when(j >= 2)
            def _():
                sum_copy(j - 2, 0).wait_send()

            def foreign(at):
                sums[j % 2, 0, at] = product(2, held.at[j], at)

            each_tile(foreign)
            sum_copy(j, 0).start()
            weight_load(j, 0).wait()
            weight_load(j, 1).wait()

            def both(at):
                acc[0, at] = product(0, held.at[j], at) + product(1, relay_w, at)
                acc[1, at] = product(1, middle_w, at)

            each_tile(both)

        @pl.when(outer)
        def _():
            def mine(at):
                acc[0, at] = product(0, held.at[j], at)

            each_tile(mine)

    def compute_cross(j):
        for b in range(blocks):
            cross_copy(j * blocks + b, True).wait_recv()

        @pl.when(inner)
        def _():
            @pl.when(j >= 2)
            def _():
                sum_copy(j - 2, 1).wait_send()

            def foreign(at):
                sums[j % 2, 1, at] = product(2, cross.at[j], at)

            each_tile(foreign)
            sum_copy(j, 1).start()

            def mine(at):
                acc[1, at] = acc[1, at] + product(0, cross.at[j], at)

            each_tile(mine)

        @pl.when(outer)
        def _():
            def mine(at):
                acc[1, at] = product(0, cross.at[j], at)

            each_tile(mine)

        shard_ref[j] = jnp.where(flipped, cross[j], held[j])

        @pl.when(outer)
        def _():
            for which in range(2):
                sum_copy(j, which).wait_recv()
                acc[which] = acc[which] + sumr[j, which]

        first, second = acc[0], acc[1]
        keys = jnp.where(own_is_key, first, second)
        values = jnp.where(own_is_key, second, first)
        turned = keys * cos_t[...] + pltpu.roll(keys, CHUNK // 2, 1) * sin_t[...]
        kv_ref[0, j] = turned.astype(kv_ref.dtype)
        kv_ref[1, j] = values.astype(kv_ref.dtype)

    def step(tau, carry):
        @pl.when(tau < steps)
        def _():
            t = tau
            old_load(t).wait()

            @pl.when(t >= 2)
            def _():
                for offset in (1, 2, 3):
                    sec_copy(t - 2, offset).wait_send()

            low, high = oldv[t % 2, 0], oldv[t % 2, 1]
            for offset in (2, 3, 1):
                send[t % 2, offset - 1] = jnp.where(target_low == section_at(offset), low, high)
            keep[t % 4] = jnp.where(target_low == sec, low, high)
            for offset in (2, 3, 1):
                sec_copy(t, offset).start()

            @pl.when(t + 2 < steps)
            def _():
                old_load(t + 2).start()

        @pl.when(outer)
        def _():
            for k in range(PIECES_PER_STEP):
                p = tau * PIECES_PER_STEP + k

                @pl.when(p < pieces)
                def _():
                    piece_copy(p).start()

        @pl.when((tau >= 2) & (tau < steps + 2))
        def _():
            t = tau - 2
            for offset in (1, 2, 3):
                sec_copy(t, offset).wait_recv()

            @pl.when(t >= 2)
            def _():
                x_copy(t - 2).wait_send()

            j, at = place_of(t)
            own, foreign = keep[t % 4], keep[t % 4]
            for offset in (1, 2, 3):
                arrived = recv[t, offset - 1]
                own = jnp.where(own_from == section_at(offset), arrived, own)
                foreign = jnp.where(foreign_from == section_at(offset), arrived, foreign)
            forv[t % 2] = foreign
            held[j, x, at] = own
            x_copy(t).start()

        @pl.when((tau >= 3) & (tau < steps + 3))
        def _():
            t = tau - 3
            x_copy(t).wait_recv()

            @pl.when(outer)
            def _():
                own_copy(t, False).start()

            @pl.when(inner)
            def _():
                own_copy(t, True).start()

        @pl.when(inner & (tau >= RETURN_LAG) & (tau < steps + RETURN_LAG))
        def _():
            t = tau - RETURN_LAG
            own_copy(t, True).wait_recv()
            cross_copy(t, False).start()

        @pl.when(inner & (tau >= CROSS_LAG) & (tau < steps + CROSS_LAG))
        def _():
            t = tau - CROSS_LAG
            own_copy(t, False).wait_recv()
            cross_copy(t, True).start()

        @pl.when(tau == 4)
        def _():
            angles()

        since = tau - first_compute + 1
        j = since // CHUNK_STEPS
        phase = since % CHUNK_STEPS
        live = (since >= 0) & (j < chunks)

        @pl.when(inner & live & (phase == 0))
        def _():
            weight_load(j, 0).start()
            weight_load(j, 1).start()

        @pl.when(live & (phase == 1))
        def _():
            compute_own(j)

        @pl.when(live & (phase == 2))
        def _():
            compute_cross(j)

        return carry

    lax.fori_loop(0, steps + CROSS_LAG + 2, step, 0)

    for t in (steps - 2, steps - 1):
        for offset in (1, 2, 3):
            sec_copy(t, offset).wait_send()
        x_copy(t).wait_send()

    def drain(t, carry):
        @pl.when(outer)
        def _():
            own_copy(t, False).wait_send()

        @pl.when(inner)
        def _():
            own_copy(t, True).wait_send()
            cross_copy(t, False).wait_send()
            cross_copy(t, True).wait_send()

        return carry

    lax.fori_loop(0, steps, drain, 0)

    @pl.when(outer)
    def _():
        def drain_piece(p, carry):
            piece_copy(p).wait_send()
            return carry

        lax.fori_loop(0, pieces, drain_piece, 0)

    for j in (chunks - 2, chunks - 1):
        @pl.when(inner)
        def _():
            for which in range(2):
                sum_copy(j, which).wait_send()


def store_kernel(held_shard, held_kv, shard_ref, kv_ref, shard_sem, kv_sem):
    chunks = held_shard.shape[0]
    kv_width = shard_ref.shape[2]
    copies = []
    for j in range(chunks):
        at = pl.ds(j * CHUNK, CHUNK)
        copies.append(
            pltpu.make_async_copy(held_shard.at[j], shard_ref.at[:, :, at], shard_sem.at[j])
        )
        for which in range(2):
            at = pl.ds(which * kv_width + j * CHUNK, CHUNK)
            copies.append(
                pltpu.make_async_copy(
                    held_kv.at[which, j], kv_ref.at[0, :, at], kv_sem.at[which, j]
                )
            )
    for copy in copies:
        copy.start()
    for copy in copies:
        copy.wait()


def per_device_chain(old_pieces, section_inputs, old_sec, new_sec, old_ord, new_ord):
    _, layers_held, rows, kv_width = old_pieces.shape
    _, tok_rows, width = section_inputs.shape
    chunks = kv_width // CHUNK
    block_rows = rows // 4
    steps = chunks * 4
    piece_rows = tok_rows // 32
    pieces = tok_rows // piece_rows
    half_dim = HEAD_DIM // 2
    index = np.arange(half_dim, dtype=np.float32)
    factor = np.float32(-2.0 * math.log(500000.0) / HEAD_DIM)
    freq = np.exp((index * factor).astype(np.float64)).astype(np.float32)
    freq = jnp.asarray(np.concatenate([freq, freq])[None])
    kind = old_pieces.dtype
    dma = pltpu.SemaphoreType.DMA
    hbm = pl.BlockSpec(memory_space=pltpu.HBM)
    smem = pl.BlockSpec(memory_space=pltpu.SMEM)
    vmem = pl.BlockSpec(memory_space=pltpu.VMEM)
    held_shard, held_kv, _, _ = pl.pallas_call(
        functools.partial(chain_kernel, block_rows, piece_rows),
        out_shape=(
            pltpu.VMEM((chunks, 2, rows, CHUNK), kind),
            pltpu.VMEM((2, chunks, tok_rows, CHUNK), kind),
            jax.ShapeDtypeStruct((chunks, 2, rows, CHUNK), kind),
            jax.ShapeDtypeStruct((chunks, 2, rows, CHUNK), kind),
        ),
        in_specs=[hbm, hbm, smem, smem, smem, smem, vmem],
        out_specs=(vmem, vmem, hbm, hbm),
        scratch_shapes=[
            pltpu.VMEM((2, layers_held, block_rows, CHUNK), kind),
            pltpu.VMEM((2, 3, block_rows, CHUNK), kind),
            pltpu.VMEM((4, block_rows, CHUNK), kind),
            pltpu.VMEM((steps, 3, block_rows, CHUNK), kind),
            pltpu.VMEM((chunks, 2, rows, CHUNK), kind),
            pltpu.VMEM((2, block_rows, CHUNK), kind),
            pltpu.VMEM((chunks, 2, rows, CHUNK), kind),
            pltpu.VMEM((3, tok_rows, width // 2), kind),
            pltpu.VMEM((tok_rows, CHUNK), jnp.float32),
            pltpu.VMEM((tok_rows, CHUNK), jnp.float32),
            pltpu.VMEM((2, rows, CHUNK), kind),
            pltpu.VMEM((2, rows, CHUNK), kind),
            pltpu.VMEM((2, 2, tok_rows, CHUNK), jnp.float32),
            pltpu.VMEM((chunks, 2, tok_rows, CHUNK), jnp.float32),
            pltpu.VMEM((2, tok_rows, CHUNK), jnp.float32),
            dma((2,)),
            dma((2, 3)),
            dma((steps, 3)),
            dma((2,)),
            dma((steps,)),
            dma((steps,)),
            dma((steps,)),
            dma((steps,)),
            dma((steps,)),
            dma((steps,)),
            dma((steps,)),
            dma((2,)),
            dma((pieces,)),
            dma((pieces,)),
            dma((2,)),
            dma((2, 2)),
            dma((chunks, 2)),
        ],
        compiler_params=pltpu.CompilerParams(
            collective_id=0, has_side_effects=True, vmem_limit_bytes=52 * 2**20
        ),
    )(old_pieces, section_inputs, old_sec, new_sec, old_ord.T, new_ord.T, freq)
    shard, kv = pl.pallas_call(
        store_kernel,
        out_shape=(
            jax.ShapeDtypeStruct((2, rows, kv_width), kind),
            jax.ShapeDtypeStruct((1, tok_rows, 2 * kv_width), kind),
        ),
        in_specs=[vmem, vmem],
        out_specs=(hbm, hbm),
        scratch_shapes=[dma((chunks,)), dma((2, chunks))],
        compiler_params=pltpu.CompilerParams(vmem_limit_bytes=2**20),
    )(held_shard, held_kv)
    return shard.reshape(1, 2 * rows, kv_width), kv


def from_partner(block, axis, stride):
    count = lax.axis_size(axis)
    route = []
    for low in range(count):
        high = low | 1 << stride
        if high != low and high < count:
            route += [(low, high), (high, low)]
    return lax.ppermute(block, axis, route)


def from_offset(block, axis, offset):
    count = lax.axis_size(axis)
    return lax.ppermute(block, axis, [(i, i ^ offset) for i in range(count)])


def rotate_keys(values, positions):
    tok_rows = values.shape[0]
    heads = values.reshape(tok_rows, -1, HEAD_DIM)
    half_dim = HEAD_DIM // 2
    freq_index = jnp.arange(half_dim, dtype=jnp.float32)
    inverse_freq = jnp.exp(freq_index * (-2.0 * math.log(500000.0) / HEAD_DIM))
    angles = positions.astype(jnp.float32)[:, None] * inverse_freq[None, :]
    cosine = jnp.cos(angles)[:, None, :]
    sine = jnp.sin(angles)[:, None, :]
    lower = heads[..., :half_dim]
    upper = heads[..., half_dim:]
    turned = jnp.concatenate(
        [lower * cosine - upper * sine, upper * cosine + lower * sine], axis=-1
    )
    return turned.reshape(tok_rows, -1)


def pick_entry(table, index_value):
    positions = jnp.arange(table.shape[0], dtype=jnp.int32)
    return jnp.sum(jnp.where(positions == index_value, table, 0))


def pick_row(table, index_value):
    positions = jnp.arange(table.shape[0], dtype=jnp.int32)[:, None]
    return jnp.sum(jnp.where(positions == index_value, table, 0), axis=0)


def chunk_columns(kv_width):
    heads = kv_width // HEAD_DIM
    edge = [1, 1] if heads >= 4 else []
    middle = heads - len(edge)
    sizes = [2] * (middle // 2) + [1] * (middle % 2) + edge
    starts = [sum(sizes[:i]) for i in range(len(sizes))]
    return [(s * HEAD_DIM, n * HEAD_DIM) for s, n in zip(starts, sizes)]


def per_device(old_pieces, section_inputs, old_section_of, new_section_of, old_order, new_order):
    section_count = lax.axis_size("section")
    member_count = lax.axis_size("fsdp")
    digit_count = member_count.bit_length() - 1
    row_index = lax.axis_index("section")
    member = lax.axis_index("fsdp")
    parity = member % 2
    layer_total = old_section_of.shape[0]
    layer_ids = jnp.arange(layer_total, dtype=jnp.int32)
    in_row = old_section_of == row_index
    layer_low = jnp.min(jnp.where(in_row, layer_ids, layer_total))
    layer_high = jnp.max(jnp.where(in_row, layer_ids, -1))
    target_low = pick_entry(new_section_of, layer_low) // 2
    layer_own = jnp.sum(jnp.where(new_section_of == 2 * row_index + parity, layer_ids, 0))
    layer_foreign = jnp.sum(jnp.where(new_section_of == 2 * row_index + 1 - parity, layer_ids, 0))
    source_own = pick_entry(old_section_of, layer_own)
    source_foreign = pick_entry(old_section_of, layer_foreign)
    pieces = old_pieces[0]
    tokens = section_inputs[0]
    tok_rows, _ = tokens.shape
    shard_rows, kv_width = 2 * pieces.shape[1], pieces.shape[2]
    own_bits = {digit: member // 2**digit % 2 for digit in range(1, digit_count)}
    own_old = pick_row(old_order, layer_own)
    own_new = pick_row(new_order, layer_own)
    flipped = own_old[0] != own_new[0]
    group_digits = digit_count - 1
    low_count = group_digits // 2
    high_digits = list(range(low_count + 1, digit_count))
    low_digits = list(range(1, low_count + 1))
    top_bit = own_bits[digit_count - 1]

    def to_groups(low, high):
        sources = []
        for offset in range(section_count):
            chosen = jnp.where(target_low == row_index ^ offset, low, high)
            if offset:
                chosen = from_offset(chosen, "section", offset)
            sources.append(chosen)
        (own_from, foreign_from, here, side), sources = lax.optimization_barrier(
            ((source_own, source_foreign, row_index, parity), sources)
        )
        own, foreign = sources[0], sources[0]
        for offset in range(1, section_count):
            own = jnp.where(own_from == here ^ offset, sources[offset], own)
            foreign = jnp.where(foreign_from == here ^ offset, sources[offset], foreign)
        partner = from_partner(foreign, "fsdp", 0)
        lower = jnp.where(side == 0, own, partner)
        upper = jnp.where(side == 0, partner, own)
        return jnp.concatenate([lower, upper], axis=-2)

    def gather_high(block):
        blocks = [block]
        for digit in high_digits:
            blocks += [from_partner(held, "fsdp", digit) for held in blocks]
        return blocks

    block_digits = high_digits[:-1]
    place_digits = block_digits[::-1] + low_digits[::-1]

    def pick_columns(flips):
        column = 0
        for digit in place_digits:
            column = 2 * column + (own_bits[digit] ^ flips[digit])
        return lax.dynamic_slice_in_dim(tokens, column * shard_rows, shard_rows, axis=1)

    row_cuts = 4 if tok_rows % 64 == 0 else 1
    token_blocks = {}
    for number in range(2 ** len(block_digits)):
        flips = {digit: number >> place & 1 for place, digit in enumerate(block_digits)}
        pending = {}
        for want in range(2**low_count):
            low_flips = {digit: want >> place & 1 for place, digit in enumerate(low_digits)}
            pending[want] = pick_columns({**flips, **low_flips})
        for place, digit in enumerate(low_digits):
            moved = dict(pending)
            for want in range(2**low_count):
                if want >> place & 1:
                    cuts = jnp.split(pending[want], row_cuts, axis=0)
                    cuts = [from_partner(cut, "fsdp", digit) for cut in cuts]
                    moved[want] = jnp.concatenate(cuts, axis=0)
            pending = moved
        for want in range(2**low_count):
            token_blocks[want, number] = pending[want]

    def project(blocks):
        sums = []
        for want in reversed(range(2**low_count)):
            for number, block in enumerate(blocks):
                product = jnp.dot(
                    token_blocks[want, number], block, preferred_element_type=jnp.float32
                )
                total = total + product if number else product
            sums.append(total)
        sums = sums[::-1]
        for place in reversed(range(low_count)):
            half = len(sums) // 2
            sums = [
                kept + from_partner(sent, "fsdp", low_digits[place])
                for kept, sent in zip(sums[:half], sums[half:])
            ]
        return sums[0]

    positions = member // 2 * tok_rows + jnp.arange(tok_rows, dtype=jnp.int32)
    shard_parts, key_parts, value_parts = [], [], []
    for number, (start, width) in enumerate(chunk_columns(kv_width)):
        part = lax.slice_in_dim(pieces, start, start + width, axis=2)
        if number == 0:
            crossed = jnp.stack(gather_high(part), axis=1)
            held = to_groups(crossed[0], crossed[1])
            blocks = [held[i] for i in range(held.shape[0])]
        else:
            blocks = gather_high(to_groups(part[0], part[1]))
        half = len(blocks) // 2
        near = project(blocks[:half])
        far = project(blocks[half:])
        shard_parts.append(jnp.where(flipped, blocks[half], blocks[0]))
        keys = jnp.where(own_old[0] == top_bit, near, far)
        values = jnp.where(own_old[1] == top_bit, near, far)
        key_parts.append(rotate_keys(keys, positions).astype(jnp.bfloat16))
        value_parts.append(values.astype(jnp.bfloat16))
    new_shard = jnp.concatenate(shard_parts, axis=1)
    joined = jnp.concatenate(key_parts + value_parts, axis=1)
    return (new_shard[None], joined[None])


def solution(mesh):
    in_specs = (P("section", None, "fsdp", None), P("section", "fsdp", None), P(), P(), P(), P())
    out_specs = (P("section", "fsdp", None), P("section", "fsdp", None))

    if dict(mesh.shape) == {"section": 4, "fsdp": 8}:
        return jax.shard_map(
            per_device_chain, mesh=mesh, in_specs=in_specs, out_specs=out_specs, check_vma=False
        )

    return jax.shard_map(
        per_device, mesh=mesh, in_specs=in_specs, out_specs=out_specs, check_vma=False
    )
```

```python
import functools
import math

import jax
import jax.numpy as jnp
import numpy as np
from jax import lax
from jax.experimental import pallas as pl
from jax.experimental.pallas import tpu as pltpu
from jax.sharding import PartitionSpec as P


HEAD_DIM = 128


CHUNK = HEAD_DIM
MESH = pl.DeviceIdType.MESH
CROSS_LAG = 11
RETURN_LAG = 6
CHUNK_STEPS = 3
PIECES_PER_STEP = 3
RAW_BLOCKS = 3
RAW_START = 12


def chain_kernel(
    block_rows, piece_rows,
    old_ref, tok_ref, old_sec, new_sec, old_ord, new_ord, freq_ref,
    shard_ref, kv_ref, relay_ref, middle_ref,
    oldv, send, keep, recv, held, forv, cross, tokv, cos_t, sin_t,
    relay_w, middle_w, sums, sumr, acc, raw, raw_send, raw_own, raw_foreign,
    old_sem, sec_send_sem, sec_recv_sem, x_send_sem, x_recv_sem, own_send_sem, relay_sem,
    middle_sem, fwd_send_sem, ret_send_sem, cross_sem, tok_sem, piece_send_sem, piece_recv_sem,
    weight_sem, sum_send_sem, sum_recv_sem,
    raw_send_sem, raw_recv_sem, raw_sec_send_sem, raw_sec_recv_sem, raw_x_send_sem, raw_x_recv_sem,
    raw_own_sem,
):
    rows = old_ref.shape[2]
    kv_width = old_ref.shape[3]
    tok_rows = tok_ref.shape[1]
    half_width = tok_ref.shape[2] // 2
    chunks = kv_width // CHUNK
    blocks = rows // block_rows
    steps = chunks * blocks
    early = steps - RAW_BLOCKS
    pieces = tok_rows // piece_rows
    layers = old_sec.shape[0]

    sec = lax.axis_index("section")
    member = lax.axis_index("fsdp")
    z, x = member // 2, member % 2
    upper = z // 2
    inner = (z == 1) | (z == 2)
    outer = (z == 0) | (z == 3)
    side = z % 2
    across = {"fsdp": (3 - z) * 2 + x}
    beside = {"fsdp": (z + 1 - 2 * side) * 2 + x}
    partner = {"fsdp": z * 2 + 1 - x}

    def section_at(offset):
        flip_core, flip_y = offset % 2, offset // 2
        core, y = sec % 2, sec // 2
        core = 1 - core if flip_core else core
        y = 1 - y if flip_y else y
        return y * 2 + core

    barrier = pltpu.get_barrier_semaphore()
    for offset in (1, 2, 3):
        pl.semaphore_signal(
            barrier, inc=1, device_id={"section": section_at(offset)}, device_id_type=MESH
        )
    pl.semaphore_signal(barrier, inc=1, device_id=partner, device_id_type=MESH)
    pl.semaphore_signal(barrier, inc=1, device_id=beside, device_id_type=MESH)

    @pl.when(inner)
    def _():
        pl.semaphore_signal(barrier, inc=1, device_id=across, device_id_type=MESH)

    def old_load(t):
        j, b = t // blocks, t % blocks
        return pltpu.make_async_copy(
            old_ref.at[0, :, pl.ds(b * block_rows, block_rows), pl.ds(j * CHUNK, CHUNK)],
            oldv.at[t % 2],
            old_sem.at[t % 2],
        )

    def tok_load(which):
        column = (side if which == 0 else 1 - side) * half_width
        return pltpu.make_async_copy(
            tok_ref.at[0, :, pl.ds(column, half_width)], tokv.at[which], tok_sem.at[which]
        )

    old_load(0).start()
    old_load(1).start()
    tok_load(0).start()
    tok_load(1).start()

    target_low = jnp.int32(0)
    own_from, foreign_from = jnp.int32(0), jnp.int32(0)
    old_first, new_first = jnp.int32(0), jnp.int32(0)
    seen = jnp.int32(0)
    for layer in range(layers):
        here = old_sec[layer] == sec
        place = new_sec[layer]
        target_low = jnp.where(here & (seen == 0), place // 2, target_low)
        seen = jnp.where(here, 1, seen)
        own_from = jnp.where(place == 2 * sec + x, old_sec[layer], own_from)
        foreign_from = jnp.where(place == 2 * sec + 1 - x, old_sec[layer], foreign_from)
        old_first = jnp.where(place == 2 * sec + x, old_ord[0, layer], old_first)
        new_first = jnp.where(place == 2 * sec + x, new_ord[0, layer], new_first)
    flipped = old_first != new_first
    own_is_key = old_first == upper

    @pl.when(inner)
    def _():
        pl.semaphore_wait(barrier, 6)

    @pl.when(outer)
    def _():
        pl.semaphore_wait(barrier, 5)

    def place_of(t):
        return t // blocks, pl.ds(pl.multiple_of((t % blocks) * block_rows, block_rows), block_rows)

    def sec_copy(t, offset):
        return pltpu.make_async_remote_copy(
            src_ref=send.at[t % 2, offset - 1],
            dst_ref=recv.at[t, offset - 1],
            send_sem=sec_send_sem.at[t % 2, offset - 1],
            recv_sem=sec_recv_sem.at[t, offset - 1],
            device_id={"section": section_at(offset)},
            device_id_type=MESH,
        )

    def x_copy(t):
        j, at = place_of(t)
        return pltpu.make_async_remote_copy(
            src_ref=forv.at[t % 2],
            dst_ref=held.at[j, x, at],
            send_sem=x_send_sem.at[t % 2],
            recv_sem=x_recv_sem.at[t],
            device_id=partner,
            device_id_type=MESH,
        )

    def own_copy(t, to_middle):
        j, at = place_of(t)
        return pltpu.make_async_remote_copy(
            src_ref=held.at[j, :, at],
            dst_ref=(middle_ref if to_middle else relay_ref).at[j, :, at],
            send_sem=own_send_sem.at[t],
            recv_sem=(middle_sem if to_middle else relay_sem).at[t],
            device_id=across if to_middle else beside,
            device_id_type=MESH,
        )

    def cross_copy(t, forward):
        j, at = place_of(t)
        return pltpu.make_async_remote_copy(
            src_ref=(relay_ref if forward else middle_ref).at[j, :, at],
            dst_ref=cross.at[j, :, at],
            send_sem=(fwd_send_sem if forward else ret_send_sem).at[t],
            recv_sem=cross_sem.at[t],
            device_id=across if forward else beside,
            device_id_type=MESH,
        )

    def raw_copy(u):
        j, at = place_of(early + u)
        return pltpu.make_async_remote_copy(
            src_ref=old_ref.at[0, :, at, pl.ds(j * CHUNK, CHUNK)],
            dst_ref=raw.at[u],
            send_sem=raw_send_sem.at[u],
            recv_sem=raw_recv_sem.at[u],
            device_id=across,
            device_id_type=MESH,
        )

    def raw_sec_copy(u, offset):
        return pltpu.make_async_remote_copy(
            src_ref=raw_send.at[offset - 1],
            dst_ref=recv.at[u, offset - 1],
            send_sem=raw_sec_send_sem.at[offset - 1],
            recv_sem=raw_sec_recv_sem.at[u, offset - 1],
            device_id={"section": section_at(offset)},
            device_id_type=MESH,
        )

    def raw_x_copy(u):
        j, at = place_of(early + u)
        return pltpu.make_async_remote_copy(
            src_ref=raw_foreign,
            dst_ref=middle_ref.at[j, x, at],
            send_sem=raw_x_send_sem,
            recv_sem=raw_x_recv_sem.at[u],
            device_id=partner,
            device_id_type=MESH,
        )

    def raw_own_copy(u):
        j, at = place_of(early + u)
        return pltpu.make_async_copy(raw_own, middle_ref.at[j, x, at], raw_own_sem)

    def piece_copy(p):
        at = pl.ds(pl.multiple_of(p * piece_rows, piece_rows), piece_rows)
        column = (1 - side) * half_width
        return pltpu.make_async_remote_copy(
            src_ref=tok_ref.at[0, at, pl.ds(column, half_width)],
            dst_ref=tokv.at[2, at],
            send_sem=piece_send_sem.at[p],
            recv_sem=piece_recv_sem.at[p],
            device_id=beside,
            device_id_type=MESH,
        )

    def sum_copy(j, which):
        return pltpu.make_async_remote_copy(
            src_ref=sums.at[j % 2, which],
            dst_ref=sumr.at[j, which],
            send_sem=sum_send_sem.at[j % 2, which],
            recv_sem=sum_recv_sem.at[j, which],
            device_id=beside,
            device_id_type=MESH,
        )

    def weight_load(j, which):
        return pltpu.make_async_copy(
            (middle_ref if which else relay_ref).at[j],
            middle_w if which else relay_w,
            weight_sem.at[which],
        )

    @pl.when(inner)
    def _():
        for u in range(RAW_BLOCKS):
            raw_copy(u).start()

    tile = min(256, tok_rows)
    tiles = tok_rows // tile

    def product(which, weights, at):
        near = jnp.dot(
            tokv[which, at, pl.ds(0, rows)], weights[0], preferred_element_type=jnp.float32
        )
        far = jnp.dot(
            tokv[which, at, pl.ds(rows, rows)], weights[1], preferred_element_type=jnp.float32
        )
        return near + far

    def each_tile(body):
        def run(i, carry):
            body(pl.ds(pl.multiple_of(i * tile, tile), tile))
            return carry

        lax.fori_loop(0, tiles, run, 0)

    def angles():
        part = min(64, tok_rows)

        def run(i, carry):
            at = pl.ds(pl.multiple_of(i * part, part), part)
            base = z * tok_rows + i * part
            position = base + lax.broadcasted_iota(jnp.int32, (part, CHUNK), 0)
            angle = position.astype(jnp.float32) * freq_ref[...]
            lane = lax.broadcasted_iota(jnp.int32, (part, CHUNK), 1)
            cos_t[at] = jnp.cos(angle)
            sine = jnp.sin(angle)
            sin_t[at] = jnp.where(lane < CHUNK // 2, -sine, sine)
            return carry

        lax.fori_loop(0, tok_rows // part, run, 0)

    first_compute = steps + CROSS_LAG - CHUNK_STEPS * (chunks - 1)

    def compute_own(j):
        @pl.when(j == 0)
        def _():
            tok_load(0).wait()
            tok_load(1).wait()

            @pl.when(inner)
            def _():
                def wait_piece(p, carry):
                    piece_copy(p).wait_recv()
                    return carry

                lax.fori_loop(0, pieces, wait_piece, 0)

        @pl.when(inner)
        def _():
            @pl.when(j >= 2)
            def _():
                sum_copy(j - 2, 0).wait_send()

            def foreign(at):
                sums[j % 2, 0, at] = product(2, held.at[j], at)

            each_tile(foreign)
            sum_copy(j, 0).start()
            weight_load(j, 0).wait()
            weight_load(j, 1).wait()

            def both(at):
                acc[0, at] = product(0, held.at[j], at) + product(1, relay_w, at)
                acc[1, at] = product(1, middle_w, at)

            each_tile(both)

        @pl.when(outer)
        def _():
            def mine(at):
                acc[0, at] = product(0, held.at[j], at)

            each_tile(mine)

    def compute_cross(j):
        for b in range(blocks):
            cross_copy(j * blocks + b, True).wait_recv()

        @pl.when(inner)
        def _():
            @pl.when(j >= 2)
            def _():
                sum_copy(j - 2, 1).wait_send()

            def foreign(at):
                sums[j % 2, 1, at] = product(2, cross.at[j], at)

            each_tile(foreign)
            sum_copy(j, 1).start()

            def mine(at):
                acc[1, at] = acc[1, at] + product(0, cross.at[j], at)

            each_tile(mine)

        @pl.when(outer)
        def _():
            def mine(at):
                acc[1, at] = product(0, cross.at[j], at)

            each_tile(mine)

        shard_ref[j] = jnp.where(flipped, cross[j], held[j])

        @pl.when(outer)
        def _():
            for which in range(2):
                sum_copy(j, which).wait_recv()
                acc[which] = acc[which] + sumr[j, which]

        first, second = acc[0], acc[1]
        keys = jnp.where(own_is_key, first, second)
        values = jnp.where(own_is_key, second, first)
        turned = keys * cos_t[...] + pltpu.roll(keys, CHUNK // 2, 1) * sin_t[...]
        kv_ref[0, j] = turned.astype(kv_ref.dtype)
        kv_ref[1, j] = values.astype(kv_ref.dtype)

    def step(tau, carry):
        @pl.when(tau < steps)
        def _():
            t = tau
            old_load(t).wait()

            @pl.when(t >= 2)
            def _():
                for offset in (1, 2, 3):
                    sec_copy(t - 2, offset).wait_send()

            low, high = oldv[t % 2, 0], oldv[t % 2, 1]
            for offset in (2, 3, 1):
                send[t % 2, offset - 1] = jnp.where(target_low == section_at(offset), low, high)
            keep[t % 3] = jnp.where(target_low == sec, low, high)
            for offset in (2, 3, 1):
                sec_copy(t, offset).start()

            @pl.when(t + 2 < steps)
            def _():
                old_load(t + 2).start()

        @pl.when(outer)
        def _():
            for k in range(PIECES_PER_STEP):
                p = tau * PIECES_PER_STEP + k

                @pl.when(p < pieces)
                def _():
                    piece_copy(p).start()

        @pl.when((tau >= 2) & (tau < steps + 2))
        def _():
            t = tau - 2
            for offset in (1, 2, 3):
                sec_copy(t, offset).wait_recv()

            @pl.when(t >= 2)
            def _():
                x_copy(t - 2).wait_send()

            j, at = place_of(t)
            own, foreign = keep[t % 3], keep[t % 3]
            for offset in (1, 2, 3):
                arrived = recv[t, offset - 1]
                own = jnp.where(own_from == section_at(offset), arrived, own)
                foreign = jnp.where(foreign_from == section_at(offset), arrived, foreign)
            forv[t % 2] = foreign
            held[j, x, at] = own
            x_copy(t).start()

        @pl.when((tau >= 3) & (tau < steps + 3))
        def _():
            t = tau - 3
            x_copy(t).wait_recv()

            @pl.when(outer)
            def _():
                own_copy(t, False).start()

            @pl.when(inner & (t < early))
            def _():
                own_copy(t, True).start()

        since_raw = tau - RAW_START
        u = since_raw // 2

        @pl.when(inner & (since_raw >= 0) & (since_raw % 2 == 0) & (u < RAW_BLOCKS))
        def _():
            raw_copy(u).wait()

            @pl.when(u >= 1)
            def _():
                for offset in (1, 2, 3):
                    raw_sec_copy(u - 1, offset).wait_send()

            low, high = raw[u, 0], raw[u, 1]
            for offset in (2, 3, 1):
                raw_send[offset - 1] = jnp.where(target_low == section_at(offset), low, high)
            for offset in (2, 3, 1):
                raw_sec_copy(u, offset).start()

        @pl.when(inner & (since_raw >= 2) & (since_raw % 2 == 0) & (u < RAW_BLOCKS + 1))
        def _():
            last = u - 1
            for offset in (1, 2, 3):
                raw_sec_copy(last, offset).wait_recv()
            kept = jnp.where(target_low == sec, raw[last, 0], raw[last, 1])
            own, foreign = kept, kept
            for offset in (1, 2, 3):
                arrived = recv[last, offset - 1]
                own = jnp.where(own_from == section_at(offset), arrived, own)
                foreign = jnp.where(foreign_from == section_at(offset), arrived, foreign)
            raw_foreign[...] = foreign
            raw_own[...] = own
            raw_x_copy(last).start()
            raw_own_copy(last).start()

        @pl.when(inner & (since_raw >= 3) & (since_raw % 2 == 1) & (u < RAW_BLOCKS + 1))
        def _():
            raw_own_copy(u - 1).wait()
            raw_x_copy(u - 1).wait()

        @pl.when(inner & (tau >= RETURN_LAG) & (tau < steps + RETURN_LAG))
        def _():
            t = tau - RETURN_LAG

            @pl.when(t < early)
            def _():
                own_copy(t, True).wait_recv()

            cross_copy(t, False).start()

        @pl.when(inner & (tau >= CROSS_LAG) & (tau < steps + CROSS_LAG))
        def _():
            t = tau - CROSS_LAG
            own_copy(t, False).wait_recv()
            cross_copy(t, True).start()

        @pl.when(tau == 4)
        def _():
            angles()

        since = tau - first_compute + 1
        j = since // CHUNK_STEPS
        phase = since % CHUNK_STEPS
        live = (since >= 0) & (j < chunks)

        @pl.when(inner & live & (phase == 0))
        def _():
            weight_load(j, 0).start()
            weight_load(j, 1).start()

        @pl.when(live & (phase == 1))
        def _():
            compute_own(j)

        @pl.when(live & (phase == 2))
        def _():
            compute_cross(j)

        return carry

    lax.fori_loop(0, steps + CROSS_LAG + 2, step, 0)

    for t in (steps - 2, steps - 1):
        for offset in (1, 2, 3):
            sec_copy(t, offset).wait_send()
        x_copy(t).wait_send()

    @pl.when(inner)
    def _():
        for offset in (1, 2, 3):
            raw_sec_copy(RAW_BLOCKS - 1, offset).wait_send()

    def drain(t, carry):
        @pl.when(outer)
        def _():
            own_copy(t, False).wait_send()

        @pl.when(inner & (t < early))
        def _():
            own_copy(t, True).wait_send()

        @pl.when(inner)
        def _():
            cross_copy(t, False).wait_send()
            cross_copy(t, True).wait_send()

        return carry

    lax.fori_loop(0, steps, drain, 0)

    @pl.when(outer)
    def _():
        def drain_piece(p, carry):
            piece_copy(p).wait_send()
            return carry

        lax.fori_loop(0, pieces, drain_piece, 0)

    for j in (chunks - 2, chunks - 1):
        @pl.when(inner)
        def _():
            for which in range(2):
                sum_copy(j, which).wait_send()


def store_kernel(held_shard, held_kv, shard_ref, kv_ref, shard_sem, kv_sem):
    chunks = held_shard.shape[0]
    kv_width = shard_ref.shape[2]
    copies = []
    for j in range(chunks):
        at = pl.ds(j * CHUNK, CHUNK)
        copies.append(
            pltpu.make_async_copy(held_shard.at[j], shard_ref.at[:, :, at], shard_sem.at[j])
        )
        for which in range(2):
            at = pl.ds(which * kv_width + j * CHUNK, CHUNK)
            copies.append(
                pltpu.make_async_copy(
                    held_kv.at[which, j], kv_ref.at[0, :, at], kv_sem.at[which, j]
                )
            )
    for copy in copies:
        copy.start()
    for copy in copies:
        copy.wait()


def per_device_chain(old_pieces, section_inputs, old_sec, new_sec, old_ord, new_ord):
    _, layers_held, rows, kv_width = old_pieces.shape
    _, tok_rows, width = section_inputs.shape
    chunks = kv_width // CHUNK
    block_rows = rows // 4
    steps = chunks * 4
    piece_rows = tok_rows // 32
    pieces = tok_rows // piece_rows
    half_dim = HEAD_DIM // 2
    index = np.arange(half_dim, dtype=np.float32)
    factor = np.float32(-2.0 * math.log(500000.0) / HEAD_DIM)
    freq = np.exp((index * factor).astype(np.float64)).astype(np.float32)
    freq = jnp.asarray(np.concatenate([freq, freq])[None])
    kind = old_pieces.dtype
    dma = pltpu.SemaphoreType.DMA
    hbm = pl.BlockSpec(memory_space=pltpu.HBM)
    smem = pl.BlockSpec(memory_space=pltpu.SMEM)
    vmem = pl.BlockSpec(memory_space=pltpu.VMEM)
    held_shard, held_kv, _, _ = pl.pallas_call(
        functools.partial(chain_kernel, block_rows, piece_rows),
        out_shape=(
            pltpu.VMEM((chunks, 2, rows, CHUNK), kind),
            pltpu.VMEM((2, chunks, tok_rows, CHUNK), kind),
            jax.ShapeDtypeStruct((chunks, 2, rows, CHUNK), kind),
            jax.ShapeDtypeStruct((chunks, 2, rows, CHUNK), kind),
        ),
        in_specs=[hbm, hbm, smem, smem, smem, smem, vmem],
        out_specs=(vmem, vmem, hbm, hbm),
        scratch_shapes=[
            pltpu.VMEM((2, layers_held, block_rows, CHUNK), kind),
            pltpu.VMEM((2, 3, block_rows, CHUNK), kind),
            pltpu.VMEM((3, block_rows, CHUNK), kind),
            pltpu.VMEM((steps, 3, block_rows, CHUNK), kind),
            pltpu.VMEM((chunks, 2, rows, CHUNK), kind),
            pltpu.VMEM((2, block_rows, CHUNK), kind),
            pltpu.VMEM((chunks, 2, rows, CHUNK), kind),
            pltpu.VMEM((3, tok_rows, width // 2), kind),
            pltpu.VMEM((tok_rows, CHUNK), jnp.float32),
            pltpu.VMEM((tok_rows, CHUNK), jnp.float32),
            pltpu.VMEM((2, rows, CHUNK), kind),
            pltpu.VMEM((2, rows, CHUNK), kind),
            pltpu.VMEM((2, 2, tok_rows, CHUNK), jnp.float32),
            pltpu.VMEM((chunks, 2, tok_rows, CHUNK), jnp.float32),
            pltpu.VMEM((2, tok_rows, CHUNK), jnp.float32),
            pltpu.VMEM((RAW_BLOCKS, layers_held, block_rows, CHUNK), kind),
            pltpu.VMEM((3, block_rows, CHUNK), kind),
            pltpu.VMEM((block_rows, CHUNK), kind),
            pltpu.VMEM((block_rows, CHUNK), kind),
            dma((2,)),
            dma((2, 3)),
            dma((steps, 3)),
            dma((2,)),
            dma((steps,)),
            dma((steps,)),
            dma((steps,)),
            dma((steps,)),
            dma((steps,)),
            dma((steps,)),
            dma((steps,)),
            dma((2,)),
            dma((pieces,)),
            dma((pieces,)),
            dma((2,)),
            dma((2, 2)),
            dma((chunks, 2)),
            dma((RAW_BLOCKS,)),
            dma((RAW_BLOCKS,)),
            dma((3,)),
            dma((RAW_BLOCKS, 3)),
            dma,
            dma((RAW_BLOCKS,)),
            dma,
        ],
        compiler_params=pltpu.CompilerParams(
            collective_id=0, has_side_effects=True, vmem_limit_bytes=107 * 2**19
        ),
    )(old_pieces, section_inputs, old_sec, new_sec, old_ord.T, new_ord.T, freq)
    shard, kv = pl.pallas_call(
        store_kernel,
        out_shape=(
            jax.ShapeDtypeStruct((2, rows, kv_width), kind),
            jax.ShapeDtypeStruct((1, tok_rows, 2 * kv_width), kind),
        ),
        in_specs=[vmem, vmem],
        out_specs=(hbm, hbm),
        scratch_shapes=[dma((chunks,)), dma((2, chunks))],
        compiler_params=pltpu.CompilerParams(vmem_limit_bytes=2**20),
    )(held_shard, held_kv)
    return shard.reshape(1, 2 * rows, kv_width), kv


def from_partner(block, axis, stride):
    count = lax.axis_size(axis)
    route = []
    for low in range(count):
        high = low | 1 << stride
        if high != low and high < count:
            route += [(low, high), (high, low)]
    return lax.ppermute(block, axis, route)


def from_offset(block, axis, offset):
    count = lax.axis_size(axis)
    return lax.ppermute(block, axis, [(i, i ^ offset) for i in range(count)])


def rotate_keys(values, positions):
    tok_rows = values.shape[0]
    heads = values.reshape(tok_rows, -1, HEAD_DIM)
    half_dim = HEAD_DIM // 2
    freq_index = jnp.arange(half_dim, dtype=jnp.float32)
    inverse_freq = jnp.exp(freq_index * (-2.0 * math.log(500000.0) / HEAD_DIM))
    angles = positions.astype(jnp.float32)[:, None] * inverse_freq[None, :]
    cosine = jnp.cos(angles)[:, None, :]
    sine = jnp.sin(angles)[:, None, :]
    lower = heads[..., :half_dim]
    upper = heads[..., half_dim:]
    turned = jnp.concatenate(
        [lower * cosine - upper * sine, upper * cosine + lower * sine], axis=-1
    )
    return turned.reshape(tok_rows, -1)


def pick_entry(table, index_value):
    positions = jnp.arange(table.shape[0], dtype=jnp.int32)
    return jnp.sum(jnp.where(positions == index_value, table, 0))


def pick_row(table, index_value):
    positions = jnp.arange(table.shape[0], dtype=jnp.int32)[:, None]
    return jnp.sum(jnp.where(positions == index_value, table, 0), axis=0)


def chunk_columns(kv_width):
    heads = kv_width // HEAD_DIM
    edge = [1, 1] if heads >= 4 else []
    middle = heads - len(edge)
    sizes = [2] * (middle // 2) + [1] * (middle % 2) + edge
    starts = [sum(sizes[:i]) for i in range(len(sizes))]
    return [(s * HEAD_DIM, n * HEAD_DIM) for s, n in zip(starts, sizes)]


def per_device(old_pieces, section_inputs, old_section_of, new_section_of, old_order, new_order):
    section_count = lax.axis_size("section")
    member_count = lax.axis_size("fsdp")
    digit_count = member_count.bit_length() - 1
    row_index = lax.axis_index("section")
    member = lax.axis_index("fsdp")
    parity = member % 2
    layer_total = old_section_of.shape[0]
    layer_ids = jnp.arange(layer_total, dtype=jnp.int32)
    in_row = old_section_of == row_index
    layer_low = jnp.min(jnp.where(in_row, layer_ids, layer_total))
    layer_high = jnp.max(jnp.where(in_row, layer_ids, -1))
    target_low = pick_entry(new_section_of, layer_low) // 2
    layer_own = jnp.sum(jnp.where(new_section_of == 2 * row_index + parity, layer_ids, 0))
    layer_foreign = jnp.sum(jnp.where(new_section_of == 2 * row_index + 1 - parity, layer_ids, 0))
    source_own = pick_entry(old_section_of, layer_own)
    source_foreign = pick_entry(old_section_of, layer_foreign)
    pieces = old_pieces[0]
    tokens = section_inputs[0]
    tok_rows, _ = tokens.shape
    shard_rows, kv_width = 2 * pieces.shape[1], pieces.shape[2]
    own_bits = {digit: member // 2**digit % 2 for digit in range(1, digit_count)}
    own_old = pick_row(old_order, layer_own)
    own_new = pick_row(new_order, layer_own)
    flipped = own_old[0] != own_new[0]
    group_digits = digit_count - 1
    low_count = group_digits // 2
    high_digits = list(range(low_count + 1, digit_count))
    low_digits = list(range(1, low_count + 1))
    top_bit = own_bits[digit_count - 1]

    def to_groups(low, high):
        sources = []
        for offset in range(section_count):
            chosen = jnp.where(target_low == row_index ^ offset, low, high)
            if offset:
                chosen = from_offset(chosen, "section", offset)
            sources.append(chosen)
        (own_from, foreign_from, here, side), sources = lax.optimization_barrier(
            ((source_own, source_foreign, row_index, parity), sources)
        )
        own, foreign = sources[0], sources[0]
        for offset in range(1, section_count):
            own = jnp.where(own_from == here ^ offset, sources[offset], own)
            foreign = jnp.where(foreign_from == here ^ offset, sources[offset], foreign)
        partner = from_partner(foreign, "fsdp", 0)
        lower = jnp.where(side == 0, own, partner)
        upper = jnp.where(side == 0, partner, own)
        return jnp.concatenate([lower, upper], axis=-2)

    def gather_high(block):
        blocks = [block]
        for digit in high_digits:
            blocks += [from_partner(held, "fsdp", digit) for held in blocks]
        return blocks

    block_digits = high_digits[:-1]
    place_digits = block_digits[::-1] + low_digits[::-1]

    def pick_columns(flips):
        column = 0
        for digit in place_digits:
            column = 2 * column + (own_bits[digit] ^ flips[digit])
        return lax.dynamic_slice_in_dim(tokens, column * shard_rows, shard_rows, axis=1)

    row_cuts = 4 if tok_rows % 64 == 0 else 1
    token_blocks = {}
    for number in range(2 ** len(block_digits)):
        flips = {digit: number >> place & 1 for place, digit in enumerate(block_digits)}
        pending = {}
        for want in range(2**low_count):
            low_flips = {digit: want >> place & 1 for place, digit in enumerate(low_digits)}
            pending[want] = pick_columns({**flips, **low_flips})
        for place, digit in enumerate(low_digits):
            moved = dict(pending)
            for want in range(2**low_count):
                if want >> place & 1:
                    cuts = jnp.split(pending[want], row_cuts, axis=0)
                    cuts = [from_partner(cut, "fsdp", digit) for cut in cuts]
                    moved[want] = jnp.concatenate(cuts, axis=0)
            pending = moved
        for want in range(2**low_count):
            token_blocks[want, number] = pending[want]

    def project(blocks):
        sums = []
        for want in reversed(range(2**low_count)):
            for number, block in enumerate(blocks):
                product = jnp.dot(
                    token_blocks[want, number], block, preferred_element_type=jnp.float32
                )
                total = total + product if number else product
            sums.append(total)
        sums = sums[::-1]
        for place in reversed(range(low_count)):
            half = len(sums) // 2
            sums = [
                kept + from_partner(sent, "fsdp", low_digits[place])
                for kept, sent in zip(sums[:half], sums[half:])
            ]
        return sums[0]

    positions = member // 2 * tok_rows + jnp.arange(tok_rows, dtype=jnp.int32)
    shard_parts, key_parts, value_parts = [], [], []
    for number, (start, width) in enumerate(chunk_columns(kv_width)):
        part = lax.slice_in_dim(pieces, start, start + width, axis=2)
        if number == 0:
            crossed = jnp.stack(gather_high(part), axis=1)
            held = to_groups(crossed[0], crossed[1])
            blocks = [held[i] for i in range(held.shape[0])]
        else:
            blocks = gather_high(to_groups(part[0], part[1]))
        half = len(blocks) // 2
        near = project(blocks[:half])
        far = project(blocks[half:])
        shard_parts.append(jnp.where(flipped, blocks[half], blocks[0]))
        keys = jnp.where(own_old[0] == top_bit, near, far)
        values = jnp.where(own_old[1] == top_bit, near, far)
        key_parts.append(rotate_keys(keys, positions).astype(jnp.bfloat16))
        value_parts.append(values.astype(jnp.bfloat16))
    new_shard = jnp.concatenate(shard_parts, axis=1)
    joined = jnp.concatenate(key_parts + value_parts, axis=1)
    return (new_shard[None], joined[None])


def solution(mesh):
    in_specs = (P("section", None, "fsdp", None), P("section", "fsdp", None), P(), P(), P(), P())
    out_specs = (P("section", "fsdp", None), P("section", "fsdp", None))

    if dict(mesh.shape) == {"section": 4, "fsdp": 8}:
        return jax.shard_map(
            per_device_chain, mesh=mesh, in_specs=in_specs, out_specs=out_specs, check_vma=False
        )

    return jax.shard_map(
        per_device, mesh=mesh, in_specs=in_specs, out_specs=out_specs, check_vma=False
    )
```

```python
import functools
import math

import jax
import jax.numpy as jnp
import numpy as np
from jax import lax
from jax.experimental import pallas as pl
from jax.experimental.pallas import tpu as pltpu
from jax.sharding import PartitionSpec as P


HEAD_DIM = 128


CHUNK = HEAD_DIM
MESH = pl.DeviceIdType.MESH
CROSS_LAG = 11
RETURN_LAG = 6
CHUNK_STEPS = 3
PIECES_PER_STEP = 3
RAW_BLOCKS = 4
RAW_START = 12
SUM_PIECES = 4


def chain_kernel(
    block_rows, piece_rows,
    old_ref, tok_ref, old_sec_ref, new_sec_ref, old_ord_ref, new_ord_ref, freq_hbm,
    shard_ref, kv_ref, relay_ref, middle_ref,
    old_sec, new_sec, old_ord, new_ord, freq_ref,
    oldv, send, keep, recv, held, forv, cross, tokv, cos_t, sin_t,
    relay_w, middle_w, sums, sumr, acc, raw_send, raw_own, raw_foreign,
    old_sem, sec_send_sem, sec_recv_sem, x_send_sem, x_recv_sem, own_send_sem, relay_sem,
    middle_sem, fwd_send_sem, ret_send_sem, cross_sem, tok_sem, piece_send_sem, piece_recv_sem,
    weight_sem, sum_send_sem, sum_recv_sem,
    raw_send_sem, raw_recv_sem, raw_sec_send_sem, raw_sec_recv_sem, raw_x_send_sem, raw_x_recv_sem,
    raw_own_sem, table_sem,
):
    rows = old_ref.shape[2]
    kv_width = old_ref.shape[3]
    tok_rows = tok_ref.shape[1]
    half_width = tok_ref.shape[2] // 2
    chunks = kv_width // CHUNK
    blocks = rows // block_rows
    steps = chunks * blocks
    early = steps - RAW_BLOCKS
    pairs = steps // 2
    chunk_pairs = blocks // 2
    part_rows = tok_rows // SUM_PIECES
    pieces = tok_rows // piece_rows
    layers = old_sec_ref.shape[0]

    sec = lax.axis_index("section")
    member = lax.axis_index("fsdp")
    z, x = member // 2, member % 2
    upper = z // 2
    inner = (z == 1) | (z == 2)
    outer = (z == 0) | (z == 3)
    side = z % 2
    across = {"fsdp": (3 - z) * 2 + x}
    beside = {"fsdp": (z + 1 - 2 * side) * 2 + x}
    partner = {"fsdp": z * 2 + 1 - x}

    def section_at(offset):
        flip_core, flip_y = offset % 2, offset // 2
        core, y = sec % 2, sec // 2
        core = 1 - core if flip_core else core
        y = 1 - y if flip_y else y
        return y * 2 + core

    barrier = pltpu.get_barrier_semaphore()
    for offset in (1, 2, 3):
        pl.semaphore_signal(
            barrier, inc=1, device_id={"section": section_at(offset)}, device_id_type=MESH
        )
    pl.semaphore_signal(barrier, inc=1, device_id=partner, device_id_type=MESH)
    pl.semaphore_signal(barrier, inc=1, device_id=beside, device_id_type=MESH)

    @pl.when(inner)
    def _():
        pl.semaphore_signal(barrier, inc=1, device_id=across, device_id_type=MESH)

    def old_load(t):
        j, b = t // blocks, t % blocks
        return pltpu.make_async_copy(
            old_ref.at[0, :, pl.ds(b * block_rows, block_rows), pl.ds(j * CHUNK, CHUNK)],
            oldv.at[t % 2],
            old_sem.at[t % 2],
        )

    def tok_load(which):
        column = (side if which == 0 else 1 - side) * half_width
        return pltpu.make_async_copy(
            tok_ref.at[0, :, pl.ds(column, half_width)], tokv.at[which], tok_sem.at[which]
        )

    tables = [
        pltpu.make_async_copy(source, target, table_sem.at[i])
        for i, (source, target) in enumerate(
            (
                (old_sec_ref, old_sec),
                (new_sec_ref, new_sec),
                (old_ord_ref, old_ord),
                (new_ord_ref, new_ord),
                (freq_hbm, freq_ref),
            )
        )
    ]
    for table in tables:
        table.start()
    old_load(0).start()
    old_load(1).start()
    tok_load(0).start()
    tok_load(1).start()

    for table in tables:
        table.wait()
    target_low = jnp.int32(0)
    own_from, foreign_from = jnp.int32(0), jnp.int32(0)
    old_first, new_first = jnp.int32(0), jnp.int32(0)
    seen = jnp.int32(0)
    for layer in range(layers):
        here = old_sec[layer] == sec
        place = new_sec[layer]
        target_low = jnp.where(here & (seen == 0), place // 2, target_low)
        seen = jnp.where(here, 1, seen)
        own_from = jnp.where(place == 2 * sec + x, old_sec[layer], own_from)
        foreign_from = jnp.where(place == 2 * sec + 1 - x, old_sec[layer], foreign_from)
        old_first = jnp.where(place == 2 * sec + x, old_ord[0, layer], old_first)
        new_first = jnp.where(place == 2 * sec + x, new_ord[0, layer], new_first)
    flipped = old_first != new_first
    own_is_key = old_first == upper

    @pl.when(inner)
    def _():
        pl.semaphore_wait(barrier, 6)

    @pl.when(outer)
    def _():
        pl.semaphore_wait(barrier, 5)

    def place_of(t):
        return t // blocks, pl.ds(pl.multiple_of((t % blocks) * block_rows, block_rows), block_rows)

    def pair_of(p):
        first = pl.multiple_of((p % chunk_pairs) * 2 * block_rows, 2 * block_rows)
        return p // chunk_pairs, pl.ds(first, 2 * block_rows)

    def sec_copy(t, offset):
        return pltpu.make_async_remote_copy(
            src_ref=send.at[t % 2, offset - 1],
            dst_ref=recv.at[t, offset - 1],
            send_sem=sec_send_sem.at[t % 2, offset - 1],
            recv_sem=sec_recv_sem.at[t, offset - 1],
            device_id={"section": section_at(offset)},
            device_id_type=MESH,
        )

    def x_copy(t):
        j, at = place_of(t)
        return pltpu.make_async_remote_copy(
            src_ref=forv.at[t % 2],
            dst_ref=held.at[j, x, at],
            send_sem=x_send_sem.at[t % 2],
            recv_sem=x_recv_sem.at[t],
            device_id=partner,
            device_id_type=MESH,
        )

    def own_copy(p, to_middle):
        j, at = pair_of(p)
        return pltpu.make_async_remote_copy(
            src_ref=held.at[j, :, at],
            dst_ref=(middle_ref if to_middle else relay_ref).at[j, :, at],
            send_sem=own_send_sem.at[p],
            recv_sem=(middle_sem if to_middle else relay_sem).at[p],
            device_id=across if to_middle else beside,
            device_id_type=MESH,
        )

    def cross_copy(p, forward):
        j, at = pair_of(p)
        return pltpu.make_async_remote_copy(
            src_ref=(relay_ref if forward else middle_ref).at[j, :, at],
            dst_ref=cross.at[j, :, at],
            send_sem=(fwd_send_sem if forward else ret_send_sem).at[p],
            recv_sem=cross_sem.at[p],
            device_id=across if forward else beside,
            device_id_type=MESH,
        )

    def raw_copy(u):
        j, at = place_of(early + u)
        return pltpu.make_async_remote_copy(
            src_ref=old_ref.at[0, :, at, pl.ds(j * CHUNK, CHUNK)],
            dst_ref=recv.at[early + u, pl.ds(0, old_ref.shape[1])],
            send_sem=raw_send_sem.at[u],
            recv_sem=raw_recv_sem.at[u],
            device_id=across,
            device_id_type=MESH,
        )

    def raw_sec_copy(u, offset):
        return pltpu.make_async_remote_copy(
            src_ref=raw_send.at[offset - 1],
            dst_ref=recv.at[u, offset - 1],
            send_sem=raw_sec_send_sem.at[offset - 1],
            recv_sem=raw_sec_recv_sem.at[u, offset - 1],
            device_id={"section": section_at(offset)},
            device_id_type=MESH,
        )

    def raw_x_copy(u):
        j, at = place_of(early + u)
        return pltpu.make_async_remote_copy(
            src_ref=raw_foreign,
            dst_ref=middle_ref.at[j, x, at],
            send_sem=raw_x_send_sem,
            recv_sem=raw_x_recv_sem.at[u],
            device_id=partner,
            device_id_type=MESH,
        )

    def raw_own_copy(u):
        j, at = place_of(early + u)
        return pltpu.make_async_copy(raw_own, middle_ref.at[j, x, at], raw_own_sem)

    def piece_copy(p):
        at = pl.ds(pl.multiple_of(p * piece_rows, piece_rows), piece_rows)
        column = (1 - side) * half_width
        return pltpu.make_async_remote_copy(
            src_ref=tok_ref.at[0, at, pl.ds(column, half_width)],
            dst_ref=tokv.at[2, at],
            send_sem=piece_send_sem.at[p],
            recv_sem=piece_recv_sem.at[p],
            device_id=beside,
            device_id_type=MESH,
        )

    def part_of(q):
        return pl.ds(pl.multiple_of(q * part_rows, part_rows), part_rows)

    def sum_copy(j, which, q):
        return pltpu.make_async_remote_copy(
            src_ref=sums.at[j % 2, which, part_of(q)],
            dst_ref=sumr.at[j, which, part_of(q)],
            send_sem=sum_send_sem.at[j % 2, which, q],
            recv_sem=sum_recv_sem.at[j, which, q],
            device_id=beside,
            device_id_type=MESH,
        )

    def weight_load(j, which):
        return pltpu.make_async_copy(
            (middle_ref if which else relay_ref).at[j],
            middle_w if which else relay_w,
            weight_sem.at[which],
        )

    @pl.when(inner)
    def _():
        for u in range(RAW_BLOCKS):
            raw_copy(u).start()

    tile = min(256, tok_rows)
    tiles = tok_rows // tile

    def product(which, weights, at):
        near = jnp.dot(
            tokv[which, at, pl.ds(0, rows)], weights[0], preferred_element_type=jnp.float32
        )
        far = jnp.dot(
            tokv[which, at, pl.ds(rows, rows)], weights[1], preferred_element_type=jnp.float32
        )
        return near + far

    def half_product(which, weights, at, half):
        count = rows // 2
        near = jnp.dot(
            tokv[which, at, pl.ds(half * count, count)],
            weights[0, pl.ds(half * count, count)],
            preferred_element_type=jnp.float32,
        )
        far = jnp.dot(
            tokv[which, at, pl.ds(rows + half * count, count)],
            weights[1, pl.ds(half * count, count)],
            preferred_element_type=jnp.float32,
        )
        return near + far

    def each_part(body):
        def run(q, carry):
            body(q)
            return carry

        lax.fori_loop(0, SUM_PIECES, run, 0)

    def each_tile(body):
        def run(i, carry):
            body(pl.ds(pl.multiple_of(i * tile, tile), tile))
            return carry

        lax.fori_loop(0, tiles, run, 0)

    def angles():
        part = min(64, tok_rows)

        def run(i, carry):
            at = pl.ds(pl.multiple_of(i * part, part), part)
            base = z * tok_rows + i * part
            position = base + lax.broadcasted_iota(jnp.int32, (part, CHUNK), 0)
            angle = position.astype(jnp.float32) * freq_ref[...]
            lane = lax.broadcasted_iota(jnp.int32, (part, CHUNK), 1)
            cos_t[at] = jnp.cos(angle)
            sine = jnp.sin(angle)
            sin_t[at] = jnp.where(lane < CHUNK // 2, -sine, sine)
            return carry

        lax.fori_loop(0, tok_rows // part, run, 0)

    first_compute = steps + CROSS_LAG - CHUNK_STEPS * (chunks - 1)

    def compute_own(j):
        @pl.when(j == 0)
        def _():
            tok_load(0).wait()
            tok_load(1).wait()

            @pl.when(inner)
            def _():
                def wait_piece(p, carry):
                    piece_copy(p).wait_recv()
                    return carry

                lax.fori_loop(0, pieces, wait_piece, 0)

        @pl.when(inner)
        def _():
            @pl.when(j >= 2)
            def _():
                each_part(lambda q: sum_copy(j - 2, 0, q).wait_send())

            def foreign(q):
                sums[j % 2, 0, part_of(q)] = product(2, held.at[j], part_of(q))
                sum_copy(j, 0, q).start()

            each_part(foreign)
            weight_load(j, 0).wait()
            weight_load(j, 1).wait()

            def both(at):
                acc[0, at] = product(0, held.at[j], at) + product(1, relay_w, at)
                acc[1, at] = product(1, middle_w, at)

            each_tile(both)

        @pl.when(outer)
        def _():
            def mine(at):
                acc[0, at] = product(0, held.at[j], at)

            each_tile(mine)

    def compute_cross(j):
        first, second = j * chunk_pairs, j * chunk_pairs + 1
        ahead = inner & (sec % 2 == 0) & (j == chunks - 1)

        @pl.when(jnp.logical_not(ahead))
        def _():
            cross_copy(first, True).wait_recv()

        @pl.when(inner)
        def _():
            @pl.when(j >= 2)
            def _():
                each_part(lambda q: sum_copy(j - 2, 1, q).wait_send())

            def early_part(at):
                sums[j % 2, 1, at] = half_product(2, cross.at[j], at, 0)

            each_tile(early_part)
            cross_copy(second, True).wait_recv()

            def late_part(q):
                at = part_of(q)
                sums[j % 2, 1, at] = sums[j % 2, 1, at] + half_product(2, cross.at[j], at, 1)
                sum_copy(j, 1, q).start()

            each_part(late_part)

            def mine(at):
                acc[1, at] = acc[1, at] + product(0, cross.at[j], at)

            each_tile(mine)

        @pl.when(outer)
        def _():
            cross_copy(second, True).wait_recv()

            def mine(at):
                acc[1, at] = product(0, cross.at[j], at)

            each_tile(mine)

        columns = pl.ds(pl.multiple_of(j * CHUNK, CHUNK), CHUNK)
        shard_ref[:, :, columns] = jnp.where(flipped, cross[j], held[j])
        value_columns = pl.ds(pl.multiple_of(kv_width + j * CHUNK, CHUNK), CHUNK)

        def finish(q):
            at = part_of(q)

            @pl.when(outer)
            def _():
                for which in range(2):
                    sum_copy(j, which, q).wait_recv()
                    acc[which, at] = acc[which, at] + sumr[j, which, at]

            lower, higher = acc[0, at], acc[1, at]
            keys = jnp.where(own_is_key, lower, higher)
            values = jnp.where(own_is_key, higher, lower)
            turned = keys * cos_t[at] + pltpu.roll(keys, CHUNK // 2, 1) * sin_t[at]
            kv_ref[at, columns] = turned.astype(kv_ref.dtype)
            kv_ref[at, value_columns] = values.astype(kv_ref.dtype)

        each_part(finish)

    def step(tau, carry):
        @pl.when(tau < steps)
        def _():
            t = tau
            old_load(t).wait()

            @pl.when(t >= 2)
            def _():
                for offset in (1, 2, 3):
                    sec_copy(t - 2, offset).wait_send()

            low, high = oldv[t % 2, 0], oldv[t % 2, 1]
            for offset in (2, 3, 1):
                send[t % 2, offset - 1] = jnp.where(target_low == section_at(offset), low, high)
            keep[t % 3] = jnp.where(target_low == sec, low, high)
            for offset in (2, 3, 1):
                sec_copy(t, offset).start()

            @pl.when(t + 2 < steps)
            def _():
                old_load(t + 2).start()

        @pl.when(outer)
        def _():
            for k in range(PIECES_PER_STEP):
                p = tau * PIECES_PER_STEP + k

                @pl.when(p < pieces)
                def _():
                    piece_copy(p).start()

        @pl.when((tau >= 2) & (tau < steps + 2))
        def _():
            t = tau - 2
            for offset in (1, 2, 3):
                sec_copy(t, offset).wait_recv()

            @pl.when(t >= 2)
            def _():
                x_copy(t - 2).wait_send()

            j, at = place_of(t)
            own, foreign = keep[t % 3], keep[t % 3]
            for offset in (1, 2, 3):
                arrived = recv[t, offset - 1]
                own = jnp.where(own_from == section_at(offset), arrived, own)
                foreign = jnp.where(foreign_from == section_at(offset), arrived, foreign)
            forv[t % 2] = foreign
            held[j, x, at] = own
            x_copy(t).start()

        @pl.when((tau >= 3) & (tau < steps + 3))
        def _():
            t = tau - 3
            x_copy(t).wait_recv()

            @pl.when(outer & (t % 2 == 1))
            def _():
                own_copy(t // 2, False).start()

            @pl.when(inner & (t % 2 == 1) & (t < early))
            def _():
                own_copy(t // 2, True).start()

        since_raw = tau - RAW_START
        u = since_raw // 2

        @pl.when(inner & (since_raw >= 0) & (since_raw % 2 == 0) & (u < RAW_BLOCKS))
        def _():
            raw_copy(u).wait()

            @pl.when(u >= 1)
            def _():
                for offset in (1, 2, 3):
                    raw_sec_copy(u - 1, offset).wait_send()

            low, high = recv[early + u, 0], recv[early + u, 1]
            for offset in (2, 3, 1):
                raw_send[offset - 1] = jnp.where(target_low == section_at(offset), low, high)
            for offset in (2, 3, 1):
                raw_sec_copy(u, offset).start()

        @pl.when(inner & (since_raw >= 2) & (since_raw % 2 == 0) & (u < RAW_BLOCKS + 1))
        def _():
            last = u - 1
            for offset in (1, 2, 3):
                raw_sec_copy(last, offset).wait_recv()
            kept = jnp.where(target_low == sec, recv[early + last, 0], recv[early + last, 1])
            own, foreign = kept, kept
            for offset in (1, 2, 3):
                arrived = recv[last, offset - 1]
                own = jnp.where(own_from == section_at(offset), arrived, own)
                foreign = jnp.where(foreign_from == section_at(offset), arrived, foreign)
            raw_foreign[...] = foreign
            raw_own[...] = own
            raw_x_copy(last).start()
            raw_own_copy(last).start()

        @pl.when(inner & (since_raw >= 3) & (since_raw % 2 == 1) & (u < RAW_BLOCKS + 1))
        def _():
            raw_own_copy(u - 1).wait()
            raw_x_copy(u - 1).wait()

        back = tau - RETURN_LAG

        @pl.when(inner & (back >= 0) & (back < steps) & (back % 2 == 1))
        def _():
            @pl.when(back < early)
            def _():
                own_copy(back // 2, True).wait_recv()

            cross_copy(back // 2, False).start()

        forth = tau - CROSS_LAG

        @pl.when(inner & (forth >= 0) & (forth < steps) & (forth % 2 == 1))
        def _():
            p = forth // 2
            own_copy(p, False).wait_recv()

            @pl.when((sec % 2 == 0) & (p == pairs - 1))
            def _():
                cross_copy(p - 1, True).wait_recv()

            cross_copy(p, True).start()

        @pl.when(tau == 4)
        def _():
            angles()

        since = tau - first_compute + 1
        j = since // CHUNK_STEPS
        phase = since % CHUNK_STEPS
        live = (since >= 0) & (j < chunks)

        @pl.when(inner & live & (phase == 0))
        def _():
            weight_load(j, 0).start()
            weight_load(j, 1).start()

        @pl.when(live & (phase == 1))
        def _():
            compute_own(j)

        @pl.when(live & (phase == 2))
        def _():
            compute_cross(j)

        return carry

    lax.fori_loop(0, steps + CROSS_LAG + 2, step, 0)

    for t in (steps - 2, steps - 1):
        for offset in (1, 2, 3):
            sec_copy(t, offset).wait_send()
        x_copy(t).wait_send()

    @pl.when(inner)
    def _():
        for offset in (1, 2, 3):
            raw_sec_copy(RAW_BLOCKS - 1, offset).wait_send()

    def drain(p, carry):
        @pl.when(outer)
        def _():
            own_copy(p, False).wait_send()

        @pl.when(inner & (2 * p < early))
        def _():
            own_copy(p, True).wait_send()

        @pl.when(inner)
        def _():
            cross_copy(p, False).wait_send()
            cross_copy(p, True).wait_send()

        return carry

    lax.fori_loop(0, pairs, drain, 0)

    @pl.when(outer)
    def _():
        def drain_piece(p, carry):
            piece_copy(p).wait_send()
            return carry

        lax.fori_loop(0, pieces, drain_piece, 0)

    for j in (chunks - 2, chunks - 1):
        @pl.when(inner)
        def _():
            for which in range(2):
                each_part(lambda q: sum_copy(j, which, q).wait_send())


def store_kernel(held_shard, held_kv, shard_ref, kv_ref, shard_sem, kv_sem):
    halves, rows = held_shard.shape[:2]
    cuts = shard_sem.shape[1]
    copies = [pltpu.make_async_copy(held_kv, kv_ref.at[0], kv_sem)]
    for half in range(halves):
        for cut in range(cuts):
            at = pl.ds(cut * (rows // cuts), rows // cuts)
            copies.append(
                pltpu.make_async_copy(
                    held_shard.at[half, at], shard_ref.at[half, at], shard_sem.at[half, cut]
                )
            )
    for copy in copies:
        copy.start()
    for copy in copies:
        copy.wait()


def per_device_chain(old_pieces, section_inputs, old_sec, new_sec, old_ord, new_ord):
    _, layers_held, rows, kv_width = old_pieces.shape
    _, tok_rows, width = section_inputs.shape
    chunks = kv_width // CHUNK
    block_rows = rows // 4
    steps = chunks * 4
    piece_rows = tok_rows // 32
    pieces = tok_rows // piece_rows
    half_dim = HEAD_DIM // 2
    index = np.arange(half_dim, dtype=np.float32)
    factor = np.float32(-2.0 * math.log(500000.0) / HEAD_DIM)
    freq = np.exp((index * factor).astype(np.float64)).astype(np.float32)
    freq = jnp.asarray(np.concatenate([freq, freq])[None])
    kind = old_pieces.dtype
    dma = pltpu.SemaphoreType.DMA
    hbm = pl.BlockSpec(memory_space=pltpu.HBM)
    vmem = pl.BlockSpec(memory_space=pltpu.VMEM)
    held_shard, held_kv, _, _ = pl.pallas_call(
        functools.partial(chain_kernel, block_rows, piece_rows),
        out_shape=(
            pltpu.VMEM((2, rows, kv_width), kind),
            pltpu.VMEM((tok_rows, 2 * kv_width), kind),
            jax.ShapeDtypeStruct((chunks, 2, rows, CHUNK), kind),
            jax.ShapeDtypeStruct((chunks, 2, rows, CHUNK), kind),
        ),
        in_specs=[hbm] * 7,
        out_specs=(vmem, vmem, hbm, hbm),
        scratch_shapes=[
            pltpu.SMEM(old_sec.shape, jnp.int32),
            pltpu.SMEM(new_sec.shape, jnp.int32),
            pltpu.SMEM(old_ord.shape[::-1], jnp.int32),
            pltpu.SMEM(new_ord.shape[::-1], jnp.int32),
            pltpu.VMEM(freq.shape, jnp.float32),
            pltpu.VMEM((2, layers_held, block_rows, CHUNK), kind),
            pltpu.VMEM((2, 3, block_rows, CHUNK), kind),
            pltpu.VMEM((3, block_rows, CHUNK), kind),
            pltpu.VMEM((steps, 3, block_rows, CHUNK), kind),
            pltpu.VMEM((chunks, 2, rows, CHUNK), kind),
            pltpu.VMEM((2, block_rows, CHUNK), kind),
            pltpu.VMEM((chunks, 2, rows, CHUNK), kind),
            pltpu.VMEM((3, tok_rows, width // 2), kind),
            pltpu.VMEM((tok_rows, CHUNK), jnp.float32),
            pltpu.VMEM((tok_rows, CHUNK), jnp.float32),
            pltpu.VMEM((2, rows, CHUNK), kind),
            pltpu.VMEM((2, rows, CHUNK), kind),
            pltpu.VMEM((2, 2, tok_rows, CHUNK), jnp.float32),
            pltpu.VMEM((chunks, 2, tok_rows, CHUNK), jnp.float32),
            pltpu.VMEM((2, tok_rows, CHUNK), jnp.float32),
            pltpu.VMEM((3, block_rows, CHUNK), kind),
            pltpu.VMEM((block_rows, CHUNK), kind),
            pltpu.VMEM((block_rows, CHUNK), kind),
            dma((2,)),
            dma((2, 3)),
            dma((steps, 3)),
            dma((2,)),
            dma((steps,)),
            dma((steps // 2,)),
            dma((steps // 2,)),
            dma((steps // 2,)),
            dma((steps // 2,)),
            dma((steps // 2,)),
            dma((steps // 2,)),
            dma((2,)),
            dma((pieces,)),
            dma((pieces,)),
            dma((2,)),
            dma((2, 2, SUM_PIECES)),
            dma((chunks, 2, SUM_PIECES)),
            dma((RAW_BLOCKS,)),
            dma((RAW_BLOCKS,)),
            dma((3,)),
            dma((RAW_BLOCKS, 3)),
            dma,
            dma((RAW_BLOCKS,)),
            dma,
            dma((5,)),
        ],
        compiler_params=pltpu.CompilerParams(
            collective_id=0, has_side_effects=True, vmem_limit_bytes=107 * 2**19
        ),
    )(old_pieces, section_inputs, old_sec, new_sec, old_ord.T, new_ord.T, freq)
    shard, kv = pl.pallas_call(
        store_kernel,
        out_shape=(
            jax.ShapeDtypeStruct((2, rows, kv_width), kind),
            jax.ShapeDtypeStruct((1, tok_rows, 2 * kv_width), kind),
        ),
        in_specs=[vmem, vmem],
        out_specs=(hbm, hbm),
        scratch_shapes=[dma((2, 4)), dma],
        compiler_params=pltpu.CompilerParams(vmem_limit_bytes=2**20),
    )(held_shard, held_kv)
    return shard.reshape(1, 2 * rows, kv_width), kv


def from_partner(block, axis, stride):
    count = lax.axis_size(axis)
    route = []
    for low in range(count):
        high = low | 1 << stride
        if high != low and high < count:
            route += [(low, high), (high, low)]
    return lax.ppermute(block, axis, route)


def from_offset(block, axis, offset):
    count = lax.axis_size(axis)
    return lax.ppermute(block, axis, [(i, i ^ offset) for i in range(count)])


def rotate_keys(values, positions):
    tok_rows = values.shape[0]
    heads = values.reshape(tok_rows, -1, HEAD_DIM)
    half_dim = HEAD_DIM // 2
    freq_index = jnp.arange(half_dim, dtype=jnp.float32)
    inverse_freq = jnp.exp(freq_index * (-2.0 * math.log(500000.0) / HEAD_DIM))
    angles = positions.astype(jnp.float32)[:, None] * inverse_freq[None, :]
    cosine = jnp.cos(angles)[:, None, :]
    sine = jnp.sin(angles)[:, None, :]
    lower = heads[..., :half_dim]
    upper = heads[..., half_dim:]
    turned = jnp.concatenate(
        [lower * cosine - upper * sine, upper * cosine + lower * sine], axis=-1
    )
    return turned.reshape(tok_rows, -1)


def pick_entry(table, index_value):
    positions = jnp.arange(table.shape[0], dtype=jnp.int32)
    return jnp.sum(jnp.where(positions == index_value, table, 0))


def pick_row(table, index_value):
    positions = jnp.arange(table.shape[0], dtype=jnp.int32)[:, None]
    return jnp.sum(jnp.where(positions == index_value, table, 0), axis=0)


def chunk_columns(kv_width):
    heads = kv_width // HEAD_DIM
    edge = [1, 1] if heads >= 4 else []
    middle = heads - len(edge)
    sizes = [2] * (middle // 2) + [1] * (middle % 2) + edge
    starts = [sum(sizes[:i]) for i in range(len(sizes))]
    return [(s * HEAD_DIM, n * HEAD_DIM) for s, n in zip(starts, sizes)]


def per_device(old_pieces, section_inputs, old_section_of, new_section_of, old_order, new_order):
    section_count = lax.axis_size("section")
    member_count = lax.axis_size("fsdp")
    digit_count = member_count.bit_length() - 1
    row_index = lax.axis_index("section")
    member = lax.axis_index("fsdp")
    parity = member % 2
    layer_total = old_section_of.shape[0]
    layer_ids = jnp.arange(layer_total, dtype=jnp.int32)
    in_row = old_section_of == row_index
    layer_low = jnp.min(jnp.where(in_row, layer_ids, layer_total))
    layer_high = jnp.max(jnp.where(in_row, layer_ids, -1))
    target_low = pick_entry(new_section_of, layer_low) // 2
    layer_own = jnp.sum(jnp.where(new_section_of == 2 * row_index + parity, layer_ids, 0))
    layer_foreign = jnp.sum(jnp.where(new_section_of == 2 * row_index + 1 - parity, layer_ids, 0))
    source_own = pick_entry(old_section_of, layer_own)
    source_foreign = pick_entry(old_section_of, layer_foreign)
    pieces = old_pieces[0]
    tokens = section_inputs[0]
    tok_rows, _ = tokens.shape
    shard_rows, kv_width = 2 * pieces.shape[1], pieces.shape[2]
    own_bits = {digit: member // 2**digit % 2 for digit in range(1, digit_count)}
    own_old = pick_row(old_order, layer_own)
    own_new = pick_row(new_order, layer_own)
    flipped = own_old[0] != own_new[0]
    group_digits = digit_count - 1
    low_count = group_digits // 2
    high_digits = list(range(low_count + 1, digit_count))
    low_digits = list(range(1, low_count + 1))
    top_bit = own_bits[digit_count - 1]

    def to_groups(low, high):
        sources = []
        for offset in range(section_count):
            chosen = jnp.where(target_low == row_index ^ offset, low, high)
            if offset:
                chosen = from_offset(chosen, "section", offset)
            sources.append(chosen)
        (own_from, foreign_from, here, side), sources = lax.optimization_barrier(
            ((source_own, source_foreign, row_index, parity), sources)
        )
        own, foreign = sources[0], sources[0]
        for offset in range(1, section_count):
            own = jnp.where(own_from == here ^ offset, sources[offset], own)
            foreign = jnp.where(foreign_from == here ^ offset, sources[offset], foreign)
        partner = from_partner(foreign, "fsdp", 0)
        lower = jnp.where(side == 0, own, partner)
        upper = jnp.where(side == 0, partner, own)
        return jnp.concatenate([lower, upper], axis=-2)

    def gather_high(block):
        blocks = [block]
        for digit in high_digits:
            blocks += [from_partner(held, "fsdp", digit) for held in blocks]
        return blocks

    block_digits = high_digits[:-1]
    place_digits = block_digits[::-1] + low_digits[::-1]

    def pick_columns(flips):
        column = 0
        for digit in place_digits:
            column = 2 * column + (own_bits[digit] ^ flips[digit])
        return lax.dynamic_slice_in_dim(tokens, column * shard_rows, shard_rows, axis=1)

    row_cuts = 4 if tok_rows % 64 == 0 else 1
    token_blocks = {}
    for number in range(2 ** len(block_digits)):
        flips = {digit: number >> place & 1 for place, digit in enumerate(block_digits)}
        pending = {}
        for want in range(2**low_count):
            low_flips = {digit: want >> place & 1 for place, digit in enumerate(low_digits)}
            pending[want] = pick_columns({**flips, **low_flips})
        for place, digit in enumerate(low_digits):
            moved = dict(pending)
            for want in range(2**low_count):
                if want >> place & 1:
                    cuts = jnp.split(pending[want], row_cuts, axis=0)
                    cuts = [from_partner(cut, "fsdp", digit) for cut in cuts]
                    moved[want] = jnp.concatenate(cuts, axis=0)
            pending = moved
        for want in range(2**low_count):
            token_blocks[want, number] = pending[want]

    def project(blocks):
        sums = []
        for want in reversed(range(2**low_count)):
            for number, block in enumerate(blocks):
                product = jnp.dot(
                    token_blocks[want, number], block, preferred_element_type=jnp.float32
                )
                total = total + product if number else product
            sums.append(total)
        sums = sums[::-1]
        for place in reversed(range(low_count)):
            half = len(sums) // 2
            sums = [
                kept + from_partner(sent, "fsdp", low_digits[place])
                for kept, sent in zip(sums[:half], sums[half:])
            ]
        return sums[0]

    positions = member // 2 * tok_rows + jnp.arange(tok_rows, dtype=jnp.int32)
    shard_parts, key_parts, value_parts = [], [], []
    for number, (start, width) in enumerate(chunk_columns(kv_width)):
        part = lax.slice_in_dim(pieces, start, start + width, axis=2)
        if number == 0:
            crossed = jnp.stack(gather_high(part), axis=1)
            held = to_groups(crossed[0], crossed[1])
            blocks = [held[i] for i in range(held.shape[0])]
        else:
            blocks = gather_high(to_groups(part[0], part[1]))
        half = len(blocks) // 2
        near = project(blocks[:half])
        far = project(blocks[half:])
        shard_parts.append(jnp.where(flipped, blocks[half], blocks[0]))
        keys = jnp.where(own_old[0] == top_bit, near, far)
        values = jnp.where(own_old[1] == top_bit, near, far)
        key_parts.append(rotate_keys(keys, positions).astype(jnp.bfloat16))
        value_parts.append(values.astype(jnp.bfloat16))
    new_shard = jnp.concatenate(shard_parts, axis=1)
    joined = jnp.concatenate(key_parts + value_parts, axis=1)
    return (new_shard[None], joined[None])


def solution(mesh):
    in_specs = (P("section", None, "fsdp", None), P("section", "fsdp", None), P(), P(), P(), P())
    out_specs = (P("section", "fsdp", None), P("section", "fsdp", None))

    if dict(mesh.shape) == {"section": 4, "fsdp": 8}:
        return jax.shard_map(
            per_device_chain, mesh=mesh, in_specs=in_specs, out_specs=out_specs, check_vma=False
        )

    return jax.shard_map(
        per_device, mesh=mesh, in_specs=in_specs, out_specs=out_specs, check_vma=False
    )
```
